8 devices in a mesh: dp: 2 (over z, y), tp: 4 (over x, core).
Axes of the slice: x: 2, y: 2, z: 1, core: 2. Of those that a mesh axis runs over, the one named last changes fastest.
Arguments:
- x: bfloat16 [12, 256, 1536], P('dp', 'tp'), parts along dimension 0
- k_cache: bfloat16 [12, 3072, 4, 128], P('dp', None, 'tp'), parts along dimension 0
- v_cache: bfloat16 [12, 3072, 4, 128], P('dp', None, 'tp'), parts along dimension 0
- prefix_len: int32 [12], P('dp'), parts along dimension 0
- valid_len: int32 [12], P('dp'), parts along dimension 0
- g_attn: bfloat16 [1536], replicated
- w_q: bfloat16 [1536, 1536], P(None, 'tp')
- b_q: bfloat16 [1536], P('tp')
- w_k: bfloat16 [1536, 512], P(None, 'tp')
- b_k: bfloat16 [512], P('tp')
- w_v: bfloat16 [1536, 512], P(None, 'tp')
- b_v: bfloat16 [512], P('tp')
- w_o: bfloat16 [1536, 1536], P('tp')
- g_mlp: bfloat16 [1536], replicated
- w_gate: bfloat16 [1536, 8960], P(None, 'tp')
- w_up: bfloat16 [1536, 8960], P(None, 'tp')
- w_down: bfloat16 [8960, 1536], P('tp')
Outputs:
- output 1: bfloat16 [12, 256, 1536], P('dp', 'tp'), parts along dimension 0
- output 2: bfloat16 [12, 3072, 4, 128], P('dp', None, 'tp'), parts along dimension 0
- output 3: bfloat16 [12, 3072, 4, 128], P('dp', None, 'tp'), parts along dimension 0
There are 2 independent parts. The reference program is written for one: setup_inputs(seed, part) draws one part's arguments, and reference() takes and returns one part's arrays. A program takes and returns all parts, laid end to end along the dimension named above; an argument that names none is the same for every part.
All inputs are finite; a program needn't handle non-finite values.
Results may differ from the reference program's by a relative error of at most 0.0167596.
Values are sent between devices in bfloat16 or wider.
A program may use at most 1 GiB of HBM per device.

```python
import jax
import jax.numpy as jnp
from jax import lax

REQUESTS = 6
CHUNK_LEN = 256
CACHE_SLOTS = 3072
MODEL_DIM = 1536
NUM_HEADS = 12
KV_HEADS = 2
KV_STORE = 4
HEAD_DIM = 128
FFN_DIM = 8960

ROPE_THETA = 1.0e6
NORM_EPS = 1.0e-6
GROUP_SIZE = NUM_HEADS // KV_STORE
KV_REPEAT = KV_STORE // KV_HEADS


def draw_lengths(key):
    keys = jax.random.split(key, 4)
    prefix = jax.random.randint(keys[0], (REQUESTS,), 0, CACHE_SLOTS - CHUNK_LEN + 1)
    valid = jax.random.randint(keys[1], (REQUESTS,), 1, CHUNK_LEN + 1)
    req_ids = jnp.arange(REQUESTS)
    longest = jax.random.randint(keys[2], (), 0, REQUESTS)
    fullest = jax.random.randint(keys[3], (), 0, REQUESTS)
    prefix = jnp.where(req_ids == longest, CACHE_SLOTS - CHUNK_LEN, prefix)
    valid = jnp.where(req_ids == fullest, CHUNK_LEN, valid)
    return prefix.astype(jnp.int32), valid.astype(jnp.int32)


def gauss(key, shape, scale):
    return jax.random.normal(key, shape, jnp.float32) * scale


def kv_copies(values, axis):
    return jnp.repeat(values, KV_REPEAT, axis=axis)


def setup_inputs(seed: int = 0, part: int = 0) -> dict:
    shared = jax.random.split(jax.random.key(seed), 12)
    local = jax.random.split(jax.random.fold_in(jax.random.key(seed + 1), part), 5)
    prefix, valid = draw_lengths(local[0])
    q_cols = NUM_HEADS * HEAD_DIM
    kv_cols = KV_STORE * HEAD_DIM
    hidden = gauss(local[1], (REQUESTS, CHUNK_LEN, MODEL_DIM), 1.0)
    k_cache = kv_copies(gauss(local[2], (REQUESTS, CACHE_SLOTS, KV_HEADS, HEAD_DIM), 1.0), 2)
    v_mean = gauss(local[3], (REQUESTS, 1, KV_HEADS, HEAD_DIM), 1.0)
    v_cache = kv_copies(v_mean + gauss(local[4], (REQUESTS, CACHE_SLOTS, KV_HEADS, HEAD_DIM), 1.5), 2)
    w_k = kv_copies(gauss(shared[3], (MODEL_DIM, KV_HEADS, HEAD_DIM), MODEL_DIM ** -0.5), 1)
    b_k = kv_copies(gauss(shared[4], (KV_HEADS, HEAD_DIM), 1.0), 0)
    w_v = kv_copies(gauss(shared[5], (MODEL_DIM, KV_HEADS, HEAD_DIM), MODEL_DIM ** -0.5), 1)
    b_v = kv_copies(gauss(shared[6], (KV_HEADS, HEAD_DIM), 1.0), 0)
    return {
        "x": hidden.astype(jnp.bfloat16),
        "k_cache": k_cache.astype(jnp.bfloat16),
        "v_cache": v_cache.astype(jnp.bfloat16),
        "prefix_len": prefix,
        "valid_len": valid,
        "g_attn": (1.0 + gauss(shared[0], (MODEL_DIM,), 0.3)).astype(jnp.bfloat16),
        "w_q": gauss(shared[1], (MODEL_DIM, q_cols), 1.5 * MODEL_DIM ** -0.5).astype(jnp.bfloat16),
        "b_q": gauss(shared[2], (q_cols,), 1.0).astype(jnp.bfloat16),
        "w_k": w_k.reshape(MODEL_DIM, kv_cols).astype(jnp.bfloat16),
        "b_k": b_k.reshape(kv_cols).astype(jnp.bfloat16),
        "w_v": w_v.reshape(MODEL_DIM, kv_cols).astype(jnp.bfloat16),
        "b_v": b_v.reshape(kv_cols).astype(jnp.bfloat16),
        "w_o": gauss(shared[7], (q_cols, MODEL_DIM), q_cols ** -0.5).astype(jnp.bfloat16),
        "g_mlp": (1.0 + gauss(shared[8], (MODEL_DIM,), 0.3)).astype(jnp.bfloat16),
        "w_gate": gauss(shared[9], (MODEL_DIM, FFN_DIM), MODEL_DIM ** -0.5).astype(jnp.bfloat16),
        "w_up": gauss(shared[10], (MODEL_DIM, FFN_DIM), MODEL_DIM ** -0.5).astype(jnp.bfloat16),
        "w_down": gauss(shared[11], (FFN_DIM, MODEL_DIM), 1.5 * FFN_DIM ** -0.5).astype(jnp.bfloat16),
    }


def rms_norm(hidden, gain):
    wide_vals = hidden.astype(jnp.float32)
    inv_rms = lax.rsqrt(jnp.mean(wide_vals * wide_vals, axis=-1, keepdims=True) + NORM_EPS)
    return (wide_vals * inv_rms * gain.astype(jnp.float32)).astype(jnp.bfloat16)


def rotate_heads(heads, positions):
    half = heads.shape[-1] // 2
    inv_freq = ROPE_THETA ** (-(jnp.arange(half, dtype=jnp.float32) * 2.0) / heads.shape[-1])
    angles = positions.astype(jnp.float32)[..., None] * inv_freq
    cos_t = jnp.cos(angles)[..., None, :]
    sin_t = jnp.sin(angles)[..., None, :]
    wide = heads.astype(jnp.float32)
    first_half = wide[..., :half]
    second_half = wide[..., half:]
    rotated = jnp.concatenate([first_half * cos_t - second_half * sin_t, second_half * cos_t + first_half * sin_t], axis=-1)
    return rotated.astype(jnp.bfloat16)


def project(hidden, weight, bias):
    total = jnp.dot(hidden, weight, preferred_element_type=jnp.float32)
    return (total + bias.astype(jnp.float32)).astype(jnp.bfloat16)


def reference(x, k_cache, v_cache, prefix_len, valid_len, g_attn, w_q, b_q, w_k, b_k, w_v, b_v, w_o, g_mlp, w_gate, w_up, w_down):
    row_ids = jnp.arange(CHUNK_LEN)
    slot_ids = jnp.arange(CACHE_SLOTS)

    def one_request(req_args):
        hidden, k_rows, v_rows, start, count = req_args
        positions = start + row_ids
        normed = rms_norm(hidden, g_attn)
        queries = rotate_heads(project(normed, w_q, b_q).reshape(CHUNK_LEN, NUM_HEADS, HEAD_DIM), positions)
        keys_new = rotate_heads(project(normed, w_k, b_k).reshape(CHUNK_LEN, KV_STORE, HEAD_DIM), positions)
        values_new = project(normed, w_v, b_v).reshape(CHUNK_LEN, KV_STORE, HEAD_DIM)
        keep = (row_ids < count)[:, None, None]
        k_old = lax.dynamic_slice_in_dim(k_rows, start, CHUNK_LEN, axis=0)
        v_old = lax.dynamic_slice_in_dim(v_rows, start, CHUNK_LEN, axis=0)
        k_rows = lax.dynamic_update_slice_in_dim(k_rows, jnp.where(keep, keys_new, k_old), start, axis=0)
        v_rows = lax.dynamic_update_slice_in_dim(v_rows, jnp.where(keep, values_new, v_old), start, axis=0)
        limit = start + jnp.minimum(row_ids, count - 1)
        visible = slot_ids[None, :] <= limit[:, None]
        query_groups = queries.reshape(CHUNK_LEN, KV_STORE, GROUP_SIZE, HEAD_DIM)

        def one_head(head_args):
            q_head, k_head, v_head = head_args
            scores = jnp.einsum("cgd,sd->gcs", q_head.astype(jnp.float32), k_head.astype(jnp.float32)) * HEAD_DIM ** -0.5
            scores = jnp.where(visible[None], scores, -1.0e30)
            attn_probs = jax.nn.softmax(scores, axis=-1).astype(jnp.bfloat16)
            mixed = jnp.einsum("gcs,sd->cgd", attn_probs.astype(jnp.float32), v_head.astype(jnp.float32))
            return mixed.astype(jnp.bfloat16)

        heads_out = lax.map(one_head, (jnp.moveaxis(query_groups, 1, 0), jnp.moveaxis(k_rows, 1, 0), jnp.moveaxis(v_rows, 1, 0)))
        attended = jnp.moveaxis(heads_out, 0, 1).reshape(CHUNK_LEN, NUM_HEADS * HEAD_DIM)
        attn_out = jnp.dot(attended, w_o, preferred_element_type=jnp.float32).astype(jnp.bfloat16)
        resid_mid = (hidden.astype(jnp.float32) + attn_out.astype(jnp.float32)).astype(jnp.bfloat16)
        normed_mlp = rms_norm(resid_mid, g_mlp)
        gate = jnp.dot(normed_mlp, w_gate, preferred_element_type=jnp.float32)
        up_proj = jnp.dot(normed_mlp, w_up, preferred_element_type=jnp.float32)
        hidden_act = (jax.nn.silu(gate) * up_proj).astype(jnp.bfloat16)
        down = jnp.dot(hidden_act, w_down, preferred_element_type=jnp.float32).astype(jnp.bfloat16)
        result = (resid_mid.astype(jnp.float32) + down.astype(jnp.float32)).astype(jnp.bfloat16)
        return result, k_rows, v_rows

    x_out, k_out, v_out = lax.map(one_request, (x, k_cache, v_cache, prefix_len, valid_len))
    return x_out, k_out, v_out
```

```python
import jax
import jax.numpy as jnp
import numpy as np
from jax import lax
from jax.experimental import pallas as pl
from jax.experimental.pallas import tpu as pltpu
from jax.sharding import PartitionSpec as P

ROPE_THETA = 1.0e6
NORM_EPS = 1.0e-6
LOG2E = 1.4426950408889634
MESH = pl.DeviceIdType.MESH
ANY = pl.BlockSpec(memory_space=pl.ANY)
VMEM = pl.BlockSpec(memory_space=pltpu.VMEM)
SMEM = pl.BlockSpec(memory_space=pltpu.SMEM)
DMA = pltpu.SemaphoreType.DMA
REQ = 6
ROWS = 64
WIDTH = 1536
HEAD = 128
FFN = 2240
FFN_PAD = 2304
FFN_TILE = 768
OUT_TILE = 768
GROUP = 3


def rms_norm(wide, gain):
    inv_rms = lax.rsqrt(jnp.mean(wide * wide, axis=-1, keepdims=True) + NORM_EPS)
    return (wide * inv_rms * gain).astype(jnp.bfloat16)


def partners():
    me = lax.axis_index("tp")
    chip, core = me // 2, me % 2
    return lax.axis_index("dp"), (me, chip * 2 + 1 - core, (1 - chip) * 2 + core, (1 - chip) * 2 + 1 - core)


def greet(devices):
    barrier = pltpu.get_barrier_semaphore()
    for device in devices:
        pl.semaphore_signal(barrier, inc=1, device_id=device, device_id_type=MESH)
    pl.semaphore_wait(barrier, len(devices))


def send(src, dst, send_sem, recv_sem, device):
    return pltpu.make_async_remote_copy(src_ref=src, dst_ref=dst, send_sem=send_sem, recv_sem=recv_sem, device_id=device, device_id_type=MESH)


def rope_tables():
    freq = ROPE_THETA ** (-(np.arange(HEAD // 2, dtype=np.float64) * 2.0) / HEAD)
    freq = np.concatenate([freq, freq])
    angles = np.arange(4 * ROWS, dtype=np.float64)[:, None] * freq
    return np.cos(angles).astype(np.float32), np.sin(angles).astype(np.float32), freq.astype(np.float32)[None]


def qkv_kernel(prefix_ref, x_ref, g_ref, bias_ref, cos_ref, sin_ref, freq_ref, wq_ref, wk_ref, wv_ref,
               q_ref, k_ref, v_ref, pair_ref,
               xbuf, wbuf, cbuf, sbuf, in_sem, w_sem, out_sem, sx, rx, sc, rc, sf, rf):
    dp, (me, core_peer, chip_peer, _) = partners()
    order = (me, core_peer, chip_peer, partners()[1][3])
    load_x = pltpu.make_async_copy(x_ref, xbuf.at[0], in_sem)
    load_x.start()
    loads = (
        pltpu.make_async_copy(wq_ref, wbuf.at[:, pl.ds(0, 384)], w_sem.at[0]),
        pltpu.make_async_copy(wk_ref, wbuf.at[:, pl.ds(384, 128)], w_sem.at[1]),
        pltpu.make_async_copy(wv_ref, wbuf.at[:, pl.ds(512, 128)], w_sem.at[2]),
    )
    for load in loads:
        load.start()
    greet([(dp, core_peer), (dp, chip_peer)])
    load_x.wait()

    def to_chip(r):
        return send(xbuf.at[0, r], xbuf.at[2, r], sx.at[r], rx.at[r], (dp, chip_peer))

    def to_core(r):
        return send(xbuf.at[0, r], xbuf.at[1, r], sc.at[r], rc.at[r], (dp, core_peer))

    def forward(r):
        return send(xbuf.at[2, r], xbuf.at[3, r], sf.at[r], rf.at[r], (dp, core_peer))

    def keep(r):
        return pltpu.make_async_copy(xbuf.at[2, r], pair_ref.at[r], out_sem.at[r])

    for r in range(REQ):
        to_chip(r).start()
    for r in range(REQ):
        to_core(r).start()
    for slot in range(4):
        rows = pl.ds(pl.multiple_of(order[slot] * ROWS, ROWS), ROWS)
        cbuf[slot * ROWS:(slot + 1) * ROWS, :] = cos_ref[rows, :]
        sbuf[slot * ROWS:(slot + 1) * ROWS, :] = sin_ref[rows, :]
    for load in loads:
        load.wait()
    lane = lax.broadcasted_iota(jnp.int32, (4 * ROWS, HEAD), 1)

    def project(r):
        wide = xbuf[:, r].reshape(4 * ROWS, WIDTH).astype(jnp.float32)
        normed = rms_norm(wide, g_ref[...].astype(jnp.float32))
        total = jnp.dot(normed, wbuf[...], preferred_element_type=jnp.float32)
        rounded = (total + bias_ref[...].astype(jnp.float32)).astype(jnp.bfloat16)
        angle = jnp.full((8, HEAD), prefix_ref[r], jnp.int32).astype(jnp.float32) * freq_ref[...]
        cos_p, sin_p = jnp.cos(angle)[:1], jnp.sin(angle)[:1]
        cos_t = cos_p * cbuf[...] - sin_p * sbuf[...]
        sin_t = sin_p * cbuf[...] + cos_p * sbuf[...]
        sin_t = jnp.where(lane < HEAD // 2, -sin_t, sin_t)
        for head in range(4):
            part = rounded[:, head * HEAD:(head + 1) * HEAD].astype(jnp.float32)
            turned = (part * cos_t + pltpu.roll(part, HEAD // 2, 1) * sin_t).astype(jnp.bfloat16)
            for slot in range(4):
                rows = pl.ds(pl.multiple_of(order[slot] * ROWS, ROWS), ROWS)
                piece = turned[slot * ROWS:(slot + 1) * ROWS]
                if head < 3:
                    q_ref[r, head, rows, :] = piece
                else:
                    k_ref[r, rows, :] = piece
        for slot in range(4):
            rows = pl.ds(pl.multiple_of(order[slot] * ROWS, ROWS), ROWS)
            v_ref[r, rows, :] = rounded[slot * ROWS:(slot + 1) * ROWS, 4 * HEAD:]

    @pl.loop(0, REQ + 1)
    def _(r):
        @pl.when(r < REQ)
        def _():
            to_chip(r).wait_recv()
            forward(r).start()
            keep(r).start()

        @pl.when(r > 0)
        def _():
            to_core(r - 1).wait_recv()
            forward(r - 1).wait_recv()
            project(r - 1)

    @pl.loop(0, REQ)
    def _(r):
        to_chip(r).wait_send()
        to_core(r).wait_send()
        forward(r).wait_send()
        keep(r).wait()


def project_rows(prefix, x_rows, g_attn, bias, w_q, w_k, w_v):
    cos_i, sin_i, freq = rope_tables()
    return pl.pallas_call(
        qkv_kernel,
        in_specs=[SMEM, ANY, VMEM, VMEM, VMEM, VMEM, VMEM, ANY, ANY, ANY],
        out_specs=[VMEM, VMEM, VMEM, ANY],
        out_shape=[
            jax.ShapeDtypeStruct((REQ, 3, 4 * ROWS, HEAD), jnp.bfloat16),
            jax.ShapeDtypeStruct((REQ, 4 * ROWS, HEAD), jnp.bfloat16),
            jax.ShapeDtypeStruct((REQ, 4 * ROWS, HEAD), jnp.bfloat16),
            jax.ShapeDtypeStruct((REQ, ROWS, WIDTH), jnp.bfloat16),
        ],
        scratch_shapes=[
            pltpu.VMEM((4, REQ, ROWS, WIDTH), jnp.bfloat16),
            pltpu.VMEM((WIDTH, 640), jnp.bfloat16),
            pltpu.VMEM((4 * ROWS, HEAD), jnp.float32),
            pltpu.VMEM((4 * ROWS, HEAD), jnp.float32),
            DMA, DMA((3,)), DMA((REQ,)),
            DMA((REQ,)), DMA((REQ,)), DMA((REQ,)), DMA((REQ,)), DMA((REQ,)), DMA((REQ,)),
        ],
        compiler_params=pltpu.CompilerParams(collective_id=0, has_side_effects=True),
        name="exchange_qkv",
    )(prefix, x_rows, g_attn[None], bias, cos_i, sin_i, freq, w_q, w_k, w_v)


BLOCK_KV = 512
WINDOW = 272


def merge_rows(old_ref, fresh_ref, out_ref, start, count):
    slots = old_ref.shape[1]
    out_ref[0] = old_ref[0]
    base = pl.multiple_of(jnp.minimum((start // 16) * 16, slots - WINDOW), 16)
    shift = start - base
    fresh = fresh_ref[0].astype(jnp.float32)
    padded = jnp.concatenate([fresh, jnp.zeros((WINDOW - fresh.shape[0], fresh.shape[1]), jnp.float32)], axis=0)
    rolled = pltpu.roll(padded, shift, 0)
    idx = lax.broadcasted_iota(jnp.int32, rolled.shape, 0) - shift
    window = out_ref[0, pl.ds(base, WINDOW), :].astype(jnp.float32)
    merged = jnp.where((idx >= 0) & (idx < count), rolled, window)
    out_ref[0, pl.ds(base, WINDOW), :] = merged.astype(jnp.bfloat16)


def attn_kernel(prefix_ref, valid_ref, q_ref, kn_ref, vn_ref, k_ref, v_ref, o_ref, ko_ref, vo_ref, acc_ref, m_ref, l_ref):
    req = pl.program_id(0)
    start = prefix_ref[req]
    count = valid_ref[req]
    merge_rows(k_ref, kn_ref, ko_ref, start, count)
    merge_rows(v_ref, vn_ref, vo_ref, start, count)
    heads, rows, dim = q_ref.shape[1:]
    factor = (dim ** -0.5) * LOG2E
    acc_ref[...] = jnp.zeros_like(acc_ref)
    l_ref[...] = jnp.zeros_like(l_ref)
    m_ref[...] = jnp.full_like(m_ref, -1.0e30)
    n_full = start // BLOCK_KV
    n_all = (start + count + BLOCK_KV - 1) // BLOCK_KV

    def step(blk, masked):
        off = pl.multiple_of(blk * BLOCK_KV, BLOCK_KV)
        keys = ko_ref[0, pl.ds(off, BLOCK_KV), :]
        vals = vo_ref[0, pl.ds(off, BLOCK_KV), :]
        if masked:
            row = lax.broadcasted_iota(jnp.int32, (rows, BLOCK_KV), 0)
            col = lax.broadcasted_iota(jnp.int32, (rows, BLOCK_KV), 1)
            visible = col + off <= start + jnp.minimum(row, count - 1)
        for h in range(heads):
            s = lax.dot_general(q_ref[0, h], keys, (((1,), (1,)), ((), ())), preferred_element_type=jnp.float32)
            if masked:
                s = jnp.where(visible, s, -1.0e30)
            m_old = m_ref[h]
            m_new = jnp.maximum(m_old, jnp.max(s, axis=1, keepdims=True) * factor)
            alpha = jnp.exp2(m_old - m_new)
            p = jnp.exp2(s * factor - m_new[:, :1])
            part = p[:, :128]
            for j in range(1, BLOCK_KV // 128):
                part = part + p[:, j * 128:(j + 1) * 128]
            l_ref[h] = l_ref[h] * alpha + part
            m_ref[h] = m_new
            acc_ref[h] = acc_ref[h] * alpha + jnp.dot(p.astype(jnp.bfloat16), vals, preferred_element_type=jnp.float32)

    @pl.loop(0, n_full)
    def _(blk):
        step(blk, False)

    @pl.loop(n_full, n_all)
    def _(blk):
        step(blk, True)

    for h in range(heads):
        total = jnp.sum(l_ref[h], axis=1, keepdims=True)
        o_ref[0, :, h * dim:(h + 1) * dim] = (acc_ref[h] / total).astype(jnp.bfloat16)


def attention(prefix, valid, q, kn, vn, k_cache, v_cache):
    n_req, heads, rows, dim = q.shape
    slots = k_cache.shape[1]
    new_spec = pl.BlockSpec((1, rows, dim), lambda r, *_: (r, 0, 0))
    cache_spec = pl.BlockSpec((1, slots, dim), lambda r, *_: (r, 0, 0))
    return pl.pallas_call(
        attn_kernel,
        grid_spec=pltpu.PrefetchScalarGridSpec(
            num_scalar_prefetch=2,
            grid=(n_req,),
            in_specs=[pl.BlockSpec((1, heads, rows, dim), lambda r, *_: (r, 0, 0, 0)), new_spec, new_spec, cache_spec, cache_spec],
            out_specs=[pl.BlockSpec((1, rows, heads * dim), lambda r, *_: (r, 0, 0)), cache_spec, cache_spec],
            scratch_shapes=[pltpu.VMEM((heads, rows, dim), jnp.float32)] * 3,
        ),
        out_shape=[
            jax.ShapeDtypeStruct((n_req, rows, heads * dim), jnp.bfloat16),
            jax.ShapeDtypeStruct(k_cache.shape, jnp.bfloat16),
            jax.ShapeDtypeStruct(v_cache.shape, jnp.bfloat16),
        ],
        compiler_params=pltpu.CompilerParams(dimension_semantics=("arbitrary",)),
        name="attention",
    )(prefix, valid, q, kn, vn, k_cache, v_cache)


def mlp_kernel(o_ref, x_ref, pair_ref, g_ref, wo_ref, wx_ref, wg_ref, wu_ref, wd_ref, out_ref,
               obuf, xin, wo, wg, wu, wd, hbuf, ubuf, psend, precv, pown, xsend, xrecv, x1buf,
               w_sem, wl_sem, in_sem, so, ro, lo, swy, rwy, swc, rwc, sh, rh, sp, rp, ss, rs):
    dp, peers = partners()
    me, core_peer, chip_peer, far_peer = peers
    other_dp = 1 - dp
    half = 192

    def cols(who):
        return pl.ds(pl.multiple_of(who * 384, 384), 384)

    def share(slot, g, s):
        block = peers[s] if slot == 0 else peers[s ^ 2]
        src = o_ref.at[pl.ds(GROUP * g, GROUP), block]
        dst = obuf.at[slot, pl.ds(GROUP * g, GROUP), :, cols(me)]
        if s == 0:
            return pltpu.make_async_copy(src, dst, lo.at[slot, g])
        return send(src, dst, so.at[slot, g, s - 1], ro.at[slot, g, s - 1], (dp, peers[s]))

    def wo_rows(block, part):
        return pl.ds(pl.multiple_of(block * 384 + part * half, half), half)

    own_rows = pl.ds(pl.multiple_of(me * 384, 384), 384)
    near = wo_rows(chip_peer, dp)
    across = wo_rows(chip_peer, other_dp)
    wo_local = (
        pltpu.make_async_copy(wo_ref, wo.at[own_rows], wl_sem.at[0]),
        pltpu.make_async_copy(wx_ref, wo.at[near], wl_sem.at[1]),
    )
    wo_dp = send(wx_ref, wo.at[near], swy, rwy, (other_dp, me))
    wo_core = (
        send(wo_ref, wo.at[own_rows], swc.at[0], rwc.at[0], (dp, core_peer)),
        send(wx_ref, wo.at[near], swc.at[1], rwc.at[1], (dp, core_peer)),
        send(wo.at[across], wo.at[across], swc.at[2], rwc.at[2], (dp, core_peer)),
    )
    weights = (
        pltpu.make_async_copy(wg_ref, wg.at[pl.ds(0, FFN)], w_sem.at[0]),
        pltpu.make_async_copy(wu_ref, wu.at[pl.ds(0, FFN)], w_sem.at[1]),
        pltpu.make_async_copy(wd_ref, wd.at[pl.ds(0, FFN)], w_sem.at[2]),
    )
    x_loads = (
        pltpu.make_async_copy(x_ref, xin.at[0], in_sem.at[0]),
        pltpu.make_async_copy(pair_ref, xin.at[1], in_sem.at[1]),
    )
    order = ((1, 0), (1, 1), (0, 0), (0, 1))

    greet([(dp, core_peer), (dp, chip_peer), (dp, far_peer), (other_dp, me)])
    wo_dp.start()
    for slot, g in order:
        for s in (2, 3, 1):
            share(slot, g, s).start()
    for copy in wo_core[:2] + wo_local:
        copy.start()
    for slot, g in order:
        share(slot, g, 0).start()
    for copy in x_loads + weights:
        copy.start()
    pad = jnp.zeros((FFN_PAD - FFN, WIDTH), jnp.bfloat16)
    for buf in (wg, wu, wd):
        buf[FFN:, :] = pad

    gain = g_ref[...].astype(jnp.float32)

    def give_h(k):
        return send(hbuf.at[k, 0], hbuf.at[k, 1], sh.at[k], rh.at[k], (dp, core_peer))

    def give_p(k):
        return send(psend.at[k], precv.at[k], sp.at[k], rp.at[k], (dp, core_peer))

    def give_s(g):
        return send(xsend.at[g], xrecv.at[g], ss.at[g], rs.at[g], (dp, chip_peer))

    def attn_out(k):
        slot, g = order[k]
        for s in (2, 3, 1):
            share(slot, g, s).wait_recv()
        share(slot, g, 0).wait()
        reqs = slice(GROUP * g, GROUP * (g + 1))
        heads = obuf[slot, reqs].reshape(GROUP * ROWS, WIDTH)
        attn = jnp.dot(heads, wo[...], preferred_element_type=jnp.float32).astype(jnp.bfloat16)
        base = xin[slot, reqs].reshape(GROUP * ROWS, WIDTH)
        mid = (base.astype(jnp.float32) + attn.astype(jnp.float32)).astype(jnp.bfloat16)
        if slot == 0:
            x1buf[g] = mid
        hbuf[k, 0] = rms_norm(mid.astype(jnp.float32), gain)
        give_h(k).start()

    def mlp(k):
        give_h(k).wait_recv()
        hidden = hbuf.at[k].reshape(2 * GROUP * ROWS, WIDTH)

        @pl.loop(0, FFN_PAD // FFN_TILE)
        def _(f):
            at = pl.ds(pl.multiple_of(f * FFN_TILE, FFN_TILE), FFN_TILE)
            nt = (((1,), (1,)), ((), ()))
            gate = lax.dot_general(hidden[...], wg[at, :], nt, preferred_element_type=jnp.float32)
            up = lax.dot_general(hidden[...], wu[at, :], nt, preferred_element_type=jnp.float32)
            ubuf[:, at] = (jax.nn.silu(gate) * up).astype(jnp.bfloat16)

        @pl.loop(0, WIDTH // OUT_TILE)
        def _(n):
            at = pl.ds(pl.multiple_of(n * OUT_TILE, OUT_TILE), OUT_TILE)
            down = jnp.dot(ubuf[...], wd[:, at], preferred_element_type=jnp.float32)
            pown[k, :, at] = down[:GROUP * ROWS]
            psend[k, :, at] = down[GROUP * ROWS:].astype(jnp.bfloat16)

        give_p(k).start()

    def combine(k):
        slot, g = order[k]
        give_p(k).wait_recv()
        total = pown[k] + precv[k].astype(jnp.float32)
        if slot == 1:
            xsend[g] = total.astype(jnp.bfloat16)
            give_s(g).start()
        else:
            give_s(g).wait_recv()
            down = (total + xrecv[g].astype(jnp.float32)).astype(jnp.bfloat16)
            out = (x1buf[g].astype(jnp.float32) + down.astype(jnp.float32)).astype(jnp.bfloat16)
            out_ref[GROUP * g:GROUP * (g + 1)] = out.reshape(GROUP, ROWS, WIDTH)

    wo_dp.wait_recv()
    wo_core[2].start()
    for copy in wo_local + x_loads:
        copy.wait()
    for copy in wo_core:
        copy.wait_recv()
    attn_out(0)
    for copy in weights:
        copy.wait()
    mlp(0)
    attn_out(1)
    attn_out(2)
    combine(0)
    mlp(1)
    attn_out(3)
    combine(1)
    mlp(2)
    mlp(3)
    combine(2)
    combine(3)
    wo_dp.wait_send()
    for copy in wo_core:
        copy.wait_send()
    for k, (slot, g) in enumerate(order):
        for s in (2, 3, 1):
            share(slot, g, s).wait_send()
        give_h(k).wait_send()
        give_p(k).wait_send()
    for g in range(2):
        give_s(g).wait_send()


def finish_layer(o, x_rows, x_pair, g_mlp, w_o, w_x, w_gate_t, w_up_t, w_down):
    block = GROUP * ROWS
    return pl.pallas_call(
        mlp_kernel,
        in_specs=[ANY, ANY, ANY, VMEM, ANY, ANY, ANY, ANY, ANY],
        out_specs=VMEM,
        out_shape=jax.ShapeDtypeStruct((REQ, ROWS, WIDTH), jnp.bfloat16),
        scratch_shapes=[
            pltpu.VMEM((2, REQ, ROWS, WIDTH), jnp.bfloat16),
            pltpu.VMEM((2, REQ, ROWS, WIDTH), jnp.bfloat16),
            pltpu.VMEM((WIDTH, WIDTH), jnp.bfloat16),
            pltpu.VMEM((FFN_PAD, WIDTH), jnp.bfloat16),
            pltpu.VMEM((FFN_PAD, WIDTH), jnp.bfloat16),
            pltpu.VMEM((FFN_PAD, WIDTH), jnp.bfloat16),
            pltpu.VMEM((4, 2, block, WIDTH), jnp.bfloat16),
            pltpu.VMEM((2 * block, FFN_PAD), jnp.bfloat16),
            pltpu.VMEM((4, block, WIDTH), jnp.bfloat16),
            pltpu.VMEM((4, block, WIDTH), jnp.bfloat16),
            pltpu.VMEM((4, block, WIDTH), jnp.float32),
            pltpu.VMEM((2, block, WIDTH), jnp.bfloat16),
            pltpu.VMEM((2, block, WIDTH), jnp.bfloat16),
            pltpu.VMEM((2, block, WIDTH), jnp.bfloat16),
            DMA((3,)), DMA((2,)), DMA((2,)),
            DMA((2, 2, 3)), DMA((2, 2, 3)), DMA((2, 2)),
            DMA, DMA, DMA((3,)), DMA((3,)),
            DMA((4,)), DMA((4,)), DMA((4,)), DMA((4,)), DMA((2,)), DMA((2,)),
        ],
        compiler_params=pltpu.CompilerParams(collective_id=1, has_side_effects=True, vmem_limit_bytes=62 * 1024 * 1024),
        name="finish_layer",
    )(o, x_rows, x_pair, g_mlp[None], w_o, w_x, w_gate_t, w_up_t, w_down)


def solution(mesh):
    row_spec = P("dp", "tp", None)
    cache_spec = P("dp", None, "tp", None)
    req_spec = P("dp")
    rep_spec = P(None)
    col_spec = P(None, "tp")
    bias_spec = P("tp")
    down_spec = P("tp", None)

    def layer(x_rows, k_cache, v_cache, prefix, valid, g_attn, w_q, b_q, w_k, b_k, w_v, b_v, w_o, g_mlp, w_gate, w_up, w_down):
        cache_shape = (REQ, k_cache.shape[1], HEAD)
        bias = jnp.concatenate([b_q, b_k, b_v])[None]
        q, k_new, v_new, x_pair = project_rows(prefix, x_rows, g_attn, bias, w_q, w_k, w_v)
        w_half = lax.dynamic_slice_in_dim(w_o, lax.axis_index("dp") * 192, 192, axis=0)
        w_half, q = lax.optimization_barrier((w_half, q))
        w_x = lax.ppermute(w_half, "tp", [(0, 2), (1, 3), (2, 0), (3, 1)])
        o, k_out, v_out = attention(prefix, valid, q, k_new, v_new, k_cache.reshape(cache_shape), v_cache.reshape(cache_shape))
        x_out = finish_layer(o.reshape(REQ, 4, ROWS, 3 * HEAD), x_rows, x_pair, g_mlp, w_o, w_x, w_gate.T, w_up.T, w_down)
        return x_out, k_out.reshape(k_cache.shape), v_out.reshape(v_cache.shape)

    in_specs = (row_spec, cache_spec, cache_spec, req_spec, req_spec, rep_spec, col_spec, bias_spec, col_spec, bias_spec, col_spec, bias_spec, down_spec, rep_spec, col_spec, col_spec, down_spec)
    return jax.shard_map(layer, mesh=mesh, in_specs=in_specs, out_specs=(row_spec, cache_spec, cache_spec), check_vma=False)
```

```python
import functools

import jax
import jax.numpy as jnp
import numpy as np
from jax import lax
from jax.experimental import pallas as pl
from jax.experimental.pallas import tpu as pltpu
from jax.sharding import PartitionSpec as P

ROPE_THETA = 1.0e6
NORM_EPS = 1.0e-6
LOG2E = 1.4426950408889634
MESH = pl.DeviceIdType.MESH
ANY = pl.BlockSpec(memory_space=pl.ANY)
VMEM = pl.BlockSpec(memory_space=pltpu.VMEM)
SMEM = pl.BlockSpec(memory_space=pltpu.SMEM)
DMA = pltpu.SemaphoreType.DMA
REQ = 6
HALF_REQ = 3
ROWS = 64
WIDTH = 1536
HEAD = 128
FFN = 2240
FFN_PAD = 2304
FFN_TILE = 768
OUT_TILE = 768
GROUP = 3
WO_FIRST = 64
WO_REST = 128


def rms_norm(wide, gain):
    inv_rms = lax.rsqrt(jnp.mean(wide * wide, axis=-1, keepdims=True) + NORM_EPS)
    return (wide * inv_rms * gain).astype(jnp.bfloat16)


def partners():
    me = lax.axis_index("tp")
    chip, core = me // 2, me % 2
    return lax.axis_index("dp"), (me, chip * 2 + 1 - core, (1 - chip) * 2 + core, (1 - chip) * 2 + 1 - core)


def greet(devices):
    barrier = pltpu.get_barrier_semaphore()
    for device in devices:
        pl.semaphore_signal(barrier, inc=1, device_id=device, device_id_type=MESH)
    pl.semaphore_wait(barrier, len(devices))


def send(src, dst, send_sem, recv_sem, device):
    return pltpu.make_async_remote_copy(src_ref=src, dst_ref=dst, send_sem=send_sem, recv_sem=recv_sem, device_id=device, device_id_type=MESH)


def rope_tables():
    freq = ROPE_THETA ** (-(np.arange(HEAD // 2, dtype=np.float64) * 2.0) / HEAD)
    freq = np.concatenate([freq, freq])
    angles = np.arange(4 * ROWS, dtype=np.float64)[:, None] * freq
    return np.cos(angles).astype(np.float32), np.sin(angles).astype(np.float32), freq.astype(np.float32)[None]


def load_weights(wq_ref, wk_ref, wv_ref, wbuf, w_sem):
    return (
        pltpu.make_async_copy(wq_ref, wbuf.at[:, pl.ds(0, 384)], w_sem.at[0]),
        pltpu.make_async_copy(wk_ref, wbuf.at[:, pl.ds(384, 128)], w_sem.at[1]),
        pltpu.make_async_copy(wv_ref, wbuf.at[:, pl.ds(512, 128)], w_sem.at[2]),
    )


def project(x, position, chip, g_ref, biases, tables, wbuf, q_ref, k_ref, v_ref, r):
    cos_ref, sin_ref, freq_ref = tables
    rows = pl.ds(pl.multiple_of(chip * 2 * ROWS, 2 * ROWS), 2 * ROWS)
    normed = rms_norm(x.astype(jnp.float32), g_ref[...].astype(jnp.float32).reshape(1, WIDTH))
    total = jnp.dot(normed, wbuf[...], preferred_element_type=jnp.float32)
    angle = jnp.full((8, HEAD), position, jnp.int32).astype(jnp.float32) * freq_ref[...]
    cos_p, sin_p = jnp.cos(angle)[:1], jnp.sin(angle)[:1]
    cos_i, sin_i = cos_ref[rows, :], sin_ref[rows, :]
    cos_t = cos_p * cos_i - sin_p * sin_i
    sin_t = sin_p * cos_i + cos_p * sin_i
    lane = lax.broadcasted_iota(jnp.int32, sin_t.shape, 1)
    sin_t = jnp.where(lane < HEAD // 2, -sin_t, sin_t)
    bias = jnp.concatenate([b[...].astype(jnp.float32).reshape(1, b.shape[0]) for b in biases], axis=1)
    rounded = (total + bias).astype(jnp.bfloat16)
    for head in range(4):
        part = rounded[:, head * HEAD:(head + 1) * HEAD].astype(jnp.float32)
        turned = (part * cos_t + pltpu.roll(part, HEAD // 2, 1) * sin_t).astype(jnp.bfloat16)
        if head < 3:
            q_ref[r, head] = turned
        else:
            k_ref[r] = turned
    v_ref[r] = rounded[:, 4 * HEAD:]


def first_kernel(prefix_ref, x_ref, g_ref, bq_ref, bk_ref, bv_ref, cos_ref, sin_ref, freq_ref, wq_ref, wk_ref, wv_ref, wo_ref,
                 qa_ref, ka_ref, va_ref, qb_ref, kb_ref, vb_ref, pair_ref, first_ref, rest_ref,
                 own, other, wbuf, wpart, in_sem, w_sem, out_sem, wo_sem, sx, rx, sc, rc, sf, rf):
    dp, (me, core_peer, chip_peer, _) = partners()
    chip, core = me // 2, me % 2
    load_x = pltpu.make_async_copy(x_ref, own.at[core], in_sem)
    load_x.start()
    loads = load_weights(wq_ref, wk_ref, wv_ref, wbuf, w_sem)
    for load in loads:
        load.start()
    load_wo = pltpu.make_async_copy(wo_ref.at[pl.ds(pl.multiple_of(dp * 192, 192), 192)], wpart, wo_sem.at[0])
    load_wo.start()
    greet([(dp, core_peer), (dp, chip_peer)])
    load_x.wait()

    def to_chip(r):
        return send(own.at[core, r], other.at[core, r], sx.at[r], rx.at[r], (dp, chip_peer))

    def to_core(r):
        return send(own.at[core, r], own.at[core, r], sc.at[r], rc.at[r], (dp, core_peer))

    def forward(r):
        return send(other.at[core, r], other.at[core, r], sf.at[r], rf.at[r], (dp, core_peer))

    def keep(r):
        return pltpu.make_async_copy(other.at[core, r], pair_ref.at[r], out_sem.at[r])

    for r in range(HALF_REQ):
        to_chip(r).start()
    for r in range(REQ):
        to_core(r).start()
    load_wo.wait()
    give_wo = (
        pltpu.make_async_copy(wpart.at[pl.ds(0, WO_FIRST)], first_ref, wo_sem.at[1]),
        pltpu.make_async_copy(wpart.at[pl.ds(WO_FIRST, WO_REST)], rest_ref, wo_sem.at[2]),
    )
    for copy in give_wo:
        copy.start()
    for load in loads:
        load.wait()
    biases = (bq_ref, bk_ref, bv_ref)
    tables = (cos_ref, sin_ref, freq_ref)

    @pl.loop(0, REQ)
    def _(r):
        to_core(r).wait_recv()
        project(own[:, r].reshape(2 * ROWS, WIDTH), prefix_ref[r], chip, g_ref, biases, tables, wbuf, qa_ref, ka_ref, va_ref, r)

    @pl.loop(0, HALF_REQ + 1)
    def _(r):
        @pl.when(r < HALF_REQ)
        def _():
            to_chip(r).wait_recv()
            forward(r).start()
            keep(r).start()

        @pl.when(r > 0)
        def _():
            forward(r - 1).wait_recv()
            project(other[:, r - 1].reshape(2 * ROWS, WIDTH), prefix_ref[r - 1], 1 - chip, g_ref, biases, tables, wbuf, qb_ref, kb_ref, vb_ref, r - 1)

    for copy in give_wo:
        copy.wait()

    @pl.loop(0, REQ)
    def _(r):
        to_core(r).wait_send()

    @pl.loop(0, HALF_REQ)
    def _(r):
        to_chip(r).wait_send()
        forward(r).wait_send()
        keep(r).wait()


def second_kernel(prefix_ref, pair_ref, g_ref, bq_ref, bk_ref, bv_ref, cos_ref, sin_ref, freq_ref, wq_ref, wk_ref, wv_ref,
                  qb_ref, kb_ref, vb_ref, other, wbuf, in_sem, w_sem, sf, rf):
    dp, (me, core_peer, _, _) = partners()
    chip, core = me // 2, me % 2

    def load(r):
        return pltpu.make_async_copy(pair_ref.at[r], other.at[core, r], in_sem.at[r])

    def forward(r):
        return send(other.at[core, r], other.at[core, r], sf.at[r], rf.at[r], (dp, core_peer))

    for r in range(HALF_REQ):
        load(r).start()
    loads = load_weights(wq_ref, wk_ref, wv_ref, wbuf, w_sem)
    for copy in loads:
        copy.start()
    greet([(dp, core_peer)])
    for r in range(HALF_REQ):
        load(r).wait()
        forward(r).start()
    for copy in loads:
        copy.wait()

    @pl.loop(0, HALF_REQ)
    def _(r):
        forward(r).wait_recv()
        project(other[:, r].reshape(2 * ROWS, WIDTH), prefix_ref[HALF_REQ + r], 1 - chip, g_ref, (bq_ref, bk_ref, bv_ref), (cos_ref, sin_ref, freq_ref), wbuf, qb_ref, kb_ref, vb_ref, r)

    @pl.loop(0, HALF_REQ)
    def _(r):
        forward(r).wait_send()


def qkv_shapes(n_req):
    return [
        jax.ShapeDtypeStruct((n_req, 3, 2 * ROWS, HEAD), jnp.bfloat16),
        jax.ShapeDtypeStruct((n_req, 2 * ROWS, HEAD), jnp.bfloat16),
        jax.ShapeDtypeStruct((n_req, 2 * ROWS, HEAD), jnp.bfloat16),
    ]


def project_first(prefix, x_rows, shared, weights, w_o):
    return pl.pallas_call(
        first_kernel,
        in_specs=[SMEM, ANY] + [VMEM] * 7 + [ANY] * 4,
        out_specs=[VMEM] * 6 + [ANY] * 3,
        out_shape=qkv_shapes(REQ) + qkv_shapes(HALF_REQ) + [
            jax.ShapeDtypeStruct((HALF_REQ, ROWS, WIDTH), jnp.bfloat16),
            jax.ShapeDtypeStruct((WO_FIRST, WIDTH), jnp.bfloat16),
            jax.ShapeDtypeStruct((WO_REST, WIDTH), jnp.bfloat16),
        ],
        scratch_shapes=[
            pltpu.VMEM((2, REQ, ROWS, WIDTH), jnp.bfloat16),
            pltpu.VMEM((2, HALF_REQ, ROWS, WIDTH), jnp.bfloat16),
            pltpu.VMEM((WIDTH, 640), jnp.bfloat16),
            pltpu.VMEM((192, WIDTH), jnp.bfloat16),
            DMA, DMA((3,)), DMA((HALF_REQ,)), DMA((3,)),
            DMA((HALF_REQ,)), DMA((HALF_REQ,)), DMA((REQ,)), DMA((REQ,)), DMA((HALF_REQ,)), DMA((HALF_REQ,)),
        ],
        compiler_params=pltpu.CompilerParams(collective_id=0, has_side_effects=True),
        cost_estimate=pl.CostEstimate(flops=2 * 10 ** 9, bytes_accessed=60 * 10 ** 6, transcendentals=0),
        name="project_first",
    )(prefix, x_rows, *shared, *weights, w_o)


def project_second(prefix, pair, shared, weights):
    return pl.pallas_call(
        second_kernel,
        in_specs=[SMEM, ANY] + [VMEM] * 7 + [ANY] * 3,
        out_specs=[VMEM] * 3,
        out_shape=qkv_shapes(HALF_REQ),
        scratch_shapes=[
            pltpu.VMEM((2, HALF_REQ, ROWS, WIDTH), jnp.bfloat16),
            pltpu.VMEM((WIDTH, 640), jnp.bfloat16),
            DMA((HALF_REQ,)), DMA((3,)), DMA((HALF_REQ,)), DMA((HALF_REQ,)),
        ],
        compiler_params=pltpu.CompilerParams(collective_id=2, has_side_effects=True),
        cost_estimate=pl.CostEstimate(flops=10 ** 9, bytes_accessed=17 * 10 ** 6, transcendentals=0),
        name="project_second",
    )(prefix, pair, *shared, *weights)


BLOCK_KV = 512
WINDOW = 272


def attn_kernel(base_req, prefix_ref, valid_ref, qa_ref, ka_ref, va_ref, qb_ref, kb_ref, vb_ref, k_ref, v_ref, *refs):
    refs = refs[-23:]
    o_ref, ko_ref, vo_ref, kbuf, vbuf, obuf, qa, ka, va, qb, kb, vb, qbuf, fbuf, acc_ref, m_ref, l_ref, even_ref, odd_ref, k_sem, v_sem, out_sem, in_sem = refs
    n_req, heads = HALF_REQ, 3
    rows, dim = 4 * ROWS, HEAD
    slots = kbuf.shape[1]
    chip = lax.axis_index("tp") // 2
    ours = pl.ds(pl.multiple_of(chip * 2 * ROWS, 2 * ROWS), 2 * ROWS)
    theirs = pl.ds(pl.multiple_of((1 - chip) * 2 * ROWS, 2 * ROWS), 2 * ROWS)
    last = slots // BLOCK_KV - 1
    factor = (dim ** -0.5) * LOG2E

    def copies(r):
        at = base_req + r
        return (
            (pltpu.make_async_copy(k_ref.at[at], kbuf.at[r], k_sem.at[r]), pltpu.make_async_copy(v_ref.at[at], vbuf.at[r], v_sem.at[r])),
            (pltpu.make_async_copy(kbuf.at[r], ko_ref.at[at], out_sem.at[0, r]), pltpu.make_async_copy(vbuf.at[r], vo_ref.at[at], out_sem.at[1, r])),
            pltpu.make_async_copy(obuf.at[r], o_ref.at[r], out_sem.at[2, r]),
        )

    half = pl.ds(base_req, HALF_REQ)
    news = (
        pltpu.make_async_copy(ka_ref.at[half], ka, in_sem.at[0]),
        pltpu.make_async_copy(kb_ref, kb, in_sem.at[1]),
        pltpu.make_async_copy(va_ref.at[half], va, in_sem.at[2]),
        pltpu.make_async_copy(vb_ref, vb, in_sem.at[3]),
        pltpu.make_async_copy(qa_ref.at[half], qa, in_sem.at[4]),
        pltpu.make_async_copy(qb_ref, qb, in_sem.at[5]),
    )

    def merge(mine, far, buf, r, start, count):
        base = pl.multiple_of(jnp.minimum((start // 16) * 16, slots - WINDOW), 16)
        shift = start - base
        fbuf[ours, :] = mine.astype(jnp.float32)
        fbuf[theirs, :] = far.astype(jnp.float32)
        rolled = pltpu.roll(fbuf[...], shift, 0)
        idx = lax.broadcasted_iota(jnp.int32, rolled.shape, 0) - shift
        window = buf[r, pl.ds(base, WINDOW), :].astype(jnp.float32)
        merged = jnp.where((idx >= 0) & (idx < count), rolled, window)
        buf[r, pl.ds(base, WINDOW), :] = merged.astype(jnp.bfloat16)

    for copy in news:
        copy.start()

    @pl.loop(0, n_req)
    def _(r):
        for load in copies(r)[0]:
            load.start()

    fbuf[rows:, :] = jnp.zeros((WINDOW - rows, dim), jnp.float32)
    for copy in news:
        copy.wait()

    @pl.loop(0, n_req)
    def _(r):
        start = prefix_ref[base_req + r]
        count = valid_ref[base_req + r]
        loads, stores, give = copies(r)
        for load in loads:
            load.wait()
        merge(ka[r], kb[r], kbuf, r, start, count)
        merge(va[r], vb[r], vbuf, r, start, count)
        for store in stores:
            store.start()
        acc_ref[...] = jnp.zeros_like(acc_ref)
        l_ref[...] = jnp.zeros_like(l_ref)
        m_ref[...] = jnp.full_like(m_ref, -1.0e30)
        n_full = start // BLOCK_KV
        n_all = (start + count + BLOCK_KV - 1) // BLOCK_KV
        for h in range(heads):
            qbuf[h, ours, :] = qa[r, h]
            qbuf[h, theirs, :] = qb[r, h]
        wide = qbuf[...].reshape(heads * rows, dim).astype(jnp.float32) * factor
        high = wide.astype(jnp.bfloat16)
        low = (wide - high.astype(jnp.float32)).astype(jnp.bfloat16)
        queries = jnp.concatenate([high, low], axis=1)

        def scores(blk, dst):
            off = pl.multiple_of(jnp.minimum(blk, last) * BLOCK_KV, BLOCK_KV)
            keys = kbuf[r, pl.ds(off, BLOCK_KV), :]
            keys = jnp.concatenate([keys, keys], axis=1)
            s = lax.dot_general(queries, keys, (((1,), (1,)), ((), ())), preferred_element_type=jnp.float32)
            dst[...] = s

        def absorb(blk, src, masked):
            off = pl.multiple_of(blk * BLOCK_KV, BLOCK_KV)
            vals = vbuf[r, pl.ds(off, BLOCK_KV), :]
            s = src[...]
            if masked:
                row = lax.broadcasted_iota(jnp.int32, (rows, BLOCK_KV), 0)
                col = lax.broadcasted_iota(jnp.int32, (rows, BLOCK_KV), 1)
                visible = col + off <= start + jnp.minimum(row, count - 1)
                s = jnp.where(jnp.concatenate([visible] * heads, axis=0), s, -1.0e30)
            m_old = m_ref[...]
            best = jnp.max(s, axis=1, keepdims=True)
            m_new = jnp.maximum(m_old, best)
            alpha = jnp.exp2(m_old - m_new)
            p = jnp.exp2(s - m_new[:, :1])
            part = p[:, :128]
            for j in range(1, BLOCK_KV // 128):
                part = part + p[:, j * 128:(j + 1) * 128]
            l_ref[...] = l_ref[...] * alpha + part
            m_ref[...] = m_new
            acc_ref[...] = acc_ref[...] * alpha + jnp.dot(p.astype(jnp.bfloat16), vals, preferred_element_type=jnp.float32)

        def step(blk, masked):
            @pl.when(blk % 2 == 0)
            def _():
                scores(blk + 1, odd_ref)
                absorb(blk, even_ref, masked)

            @pl.when(blk % 2 == 1)
            def _():
                scores(blk + 1, even_ref)
                absorb(blk, odd_ref, masked)

        scores(0, even_ref)

        @pl.loop(0, n_full)
        def _(blk):
            step(blk, False)

        @pl.loop(n_full, n_all)
        def _(blk):
            step(blk, True)

        for h in range(heads):
            at = slice(h * rows, (h + 1) * rows)
            total = jnp.sum(l_ref[at], axis=1, keepdims=True)
            obuf[r, :, h * dim:(h + 1) * dim] = (acc_ref[at] / total).astype(jnp.bfloat16)
        give.start()

    @pl.loop(0, n_req)
    def _(r):
        _, stores, give = copies(r)
        for store in stores:
            store.wait()
        give.wait()


def attention(base_req, prefix, valid, mine, far, k_cache, v_cache, previous=()):
    part = (HALF_REQ, 2 * ROWS, HEAD)
    state = pltpu.VMEM((3 * 4 * ROWS, HEAD), jnp.float32)
    tile = pltpu.VMEM((3 * 4 * ROWS, BLOCK_KV), jnp.float32)
    slots = pltpu.VMEM((HALF_REQ,) + k_cache.shape[1:], jnp.bfloat16)
    q_part = pltpu.VMEM((HALF_REQ, 3, 2 * ROWS, HEAD), jnp.bfloat16)
    kv_part = pltpu.VMEM(part, jnp.bfloat16)
    return pl.pallas_call(
        functools.partial(attn_kernel, base_req),
        in_specs=[SMEM, SMEM] + [ANY] * (8 + len(previous)),
        out_specs=[ANY, ANY, ANY],
        scratch_shapes=[
            slots, slots, pltpu.VMEM((HALF_REQ, 4 * ROWS, 3 * HEAD), jnp.bfloat16),
            q_part, kv_part, kv_part, q_part, kv_part, kv_part,
            pltpu.VMEM((3, 4 * ROWS, HEAD), jnp.bfloat16),
            pltpu.VMEM((WINDOW, HEAD), jnp.float32),
            state, state, state, tile, tile,
            DMA((HALF_REQ,)), DMA((HALF_REQ,)), DMA((3, HALF_REQ)), DMA((6,)),
        ],
        out_shape=[
            jax.ShapeDtypeStruct((HALF_REQ, 4 * ROWS, 3 * HEAD), jnp.bfloat16),
            jax.ShapeDtypeStruct(k_cache.shape, jnp.bfloat16),
            jax.ShapeDtypeStruct(v_cache.shape, jnp.bfloat16),
        ],
        input_output_aliases={10 + i: 1 + i for i in range(len(previous))},
        cost_estimate=pl.CostEstimate(flops=10 ** 10, bytes_accessed=40 * 10 ** 6, transcendentals=7 * 10 ** 6),
        name="attention",
    )(prefix, valid, *mine, *far, k_cache, v_cache, *previous)


def mlp_kernel(o0_ref, o1_ref, x_ref, pair0_ref, pair1_ref, g_ref, wo_ref, near0_ref, across0_ref, near1_ref, wg_ref, wu_ref, wd_ref, out_ref,
               obuf, xin, wo, wg, wu, wd, hbuf, ubuf, psend, precv, pown, xsend, xrecv, x1buf,
               w_sem, wl_sem, in_sem, so, ro, lo, swy, rwy, swc, rwc, sh, rh, sp, rp, ss, rs):
    dp, peers = partners()
    me, core_peer, chip_peer, far_peer = peers
    other_dp = 1 - dp

    def cols(who):
        return pl.ds(pl.multiple_of(who * 384, 384), 384)

    def share(slot, g, s):
        block = peers[s] if slot == 0 else peers[s ^ 2]
        src = (o0_ref, o1_ref)[g].at[:, block]
        dst = obuf.at[slot, pl.ds(GROUP * g, GROUP), :, cols(me)]
        if s == 0:
            return pltpu.make_async_copy(src, dst, lo.at[slot, g])
        return send(src, dst, so.at[slot, g, s - 1], ro.at[slot, g, s - 1], (dp, peers[s]))

    def wo_rows(part, late):
        first = chip_peer * 384 + part * 192 + (WO_FIRST if late else 0)
        return wo.at[pl.ds(pl.multiple_of(first, 64), WO_REST if late else WO_FIRST)]

    own_rows = wo.at[pl.ds(pl.multiple_of(me * 384, 384), 384)]
    have = ((wo_ref, own_rows), (near0_ref, wo_rows(dp, False)), (across0_ref, wo_rows(other_dp, False)), (near1_ref, wo_rows(dp, True)))
    wo_local = tuple(pltpu.make_async_copy(src, dst, wl_sem.at[i]) for i, (src, dst) in enumerate(have))
    wo_dp = send(near1_ref, wo_rows(dp, True), swy, rwy, (other_dp, me))
    wo_core = tuple(send(src, dst, swc.at[i], rwc.at[i], (dp, core_peer)) for i, (src, dst) in enumerate(have))
    wo_last = send(wo_rows(other_dp, True), wo_rows(other_dp, True), swc.at[4], rwc.at[4], (dp, core_peer))
    weights = (
        pltpu.make_async_copy(wg_ref, wg.at[pl.ds(0, FFN)], w_sem.at[0]),
        pltpu.make_async_copy(wu_ref, wu.at[pl.ds(0, FFN)], w_sem.at[1]),
        pltpu.make_async_copy(wd_ref, wd.at[pl.ds(0, FFN)], w_sem.at[2]),
    )
    x_loads = (
        pltpu.make_async_copy(x_ref, xin.at[0], in_sem.at[0]),
        pltpu.make_async_copy(pair0_ref, xin.at[1, pl.ds(0, GROUP)], in_sem.at[1]),
        pltpu.make_async_copy(pair1_ref, xin.at[1, pl.ds(GROUP, GROUP)], in_sem.at[2]),
    )
    order = ((1, 0), (1, 1), (0, 0), (0, 1))

    greet([(dp, core_peer), (dp, chip_peer), (dp, far_peer), (other_dp, me)])
    wo_dp.start()
    for slot, g in order:
        for s in (2, 3, 1):
            share(slot, g, s).start()
    for copy in wo_core + wo_local:
        copy.start()
    for slot, g in order:
        share(slot, g, 0).start()
    for copy in x_loads + weights:
        copy.start()
    pad = jnp.zeros((FFN_PAD - FFN, WIDTH), jnp.bfloat16)
    for buf in (wg, wu, wd):
        buf[FFN:, :] = pad

    gain = g_ref[...].astype(jnp.float32).reshape(1, WIDTH)

    def give_h(k):
        return send(hbuf.at[k, 0], hbuf.at[k, 1], sh.at[k], rh.at[k], (dp, core_peer))

    def give_p(k):
        return send(psend.at[k], precv.at[k], sp.at[k], rp.at[k], (dp, core_peer))

    def give_s(g):
        return send(xsend.at[g], xrecv.at[g], ss.at[g], rs.at[g], (dp, chip_peer))

    def attn_out(k):
        slot, g = order[k]
        for s in (2, 3, 1):
            share(slot, g, s).wait_recv()
        share(slot, g, 0).wait()
        reqs = slice(GROUP * g, GROUP * (g + 1))
        heads = obuf[slot, reqs].reshape(GROUP * ROWS, WIDTH)
        attn = jnp.dot(heads, wo[...], preferred_element_type=jnp.float32).astype(jnp.bfloat16)
        base = xin[slot, reqs].reshape(GROUP * ROWS, WIDTH)
        mid = (base.astype(jnp.float32) + attn.astype(jnp.float32)).astype(jnp.bfloat16)
        if slot == 0:
            x1buf[g] = mid
        hbuf[k, 0] = rms_norm(mid.astype(jnp.float32), gain)
        give_h(k).start()

    def mlp(k):
        give_h(k).wait_recv()
        hidden = hbuf.at[k].reshape(2 * GROUP * ROWS, WIDTH)

        @pl.loop(0, FFN_PAD // FFN_TILE)
        def _(f):
            at = pl.ds(pl.multiple_of(f * FFN_TILE, FFN_TILE), FFN_TILE)
            nt = (((1,), (1,)), ((), ()))
            gate = lax.dot_general(hidden[...], wg[at, :], nt, preferred_element_type=jnp.float32)
            up = lax.dot_general(hidden[...], wu[at, :], nt, preferred_element_type=jnp.float32)
            ubuf[:, at] = (jax.nn.silu(gate) * up).astype(jnp.bfloat16)

        @pl.loop(0, WIDTH // OUT_TILE)
        def _(n):
            at = pl.ds(pl.multiple_of(n * OUT_TILE, OUT_TILE), OUT_TILE)
            down = jnp.dot(ubuf[...], wd[:, at], preferred_element_type=jnp.float32)
            pown[k, :, at] = down[:GROUP * ROWS]
            psend[k, :, at] = down[GROUP * ROWS:].astype(jnp.bfloat16)

        give_p(k).start()

    def combine(k):
        slot, g = order[k]
        give_p(k).wait_recv()
        total = pown[k] + precv[k].astype(jnp.float32)
        if slot == 1:
            xsend[g] = total.astype(jnp.bfloat16)
            give_s(g).start()
        else:
            give_s(g).wait_recv()
            down = (total + xrecv[g].astype(jnp.float32)).astype(jnp.bfloat16)
            out = (x1buf[g].astype(jnp.float32) + down.astype(jnp.float32)).astype(jnp.bfloat16)
            out_ref[GROUP * g:GROUP * (g + 1)] = out.reshape(GROUP, ROWS, WIDTH)

    wo_dp.wait_recv()
    wo_last.start()
    for copy in wo_local + x_loads:
        copy.wait()
    for copy in wo_core + (wo_last,):
        copy.wait_recv()
    attn_out(0)
    for copy in weights:
        copy.wait()
    mlp(0)
    attn_out(1)
    attn_out(2)
    combine(0)
    mlp(1)
    attn_out(3)
    combine(1)
    mlp(2)
    mlp(3)
    combine(2)
    combine(3)
    wo_dp.wait_send()
    for copy in wo_core + (wo_last,):
        copy.wait_send()
    for k, (slot, g) in enumerate(order):
        for s in (2, 3, 1):
            share(slot, g, s).wait_send()
        give_h(k).wait_send()
        give_p(k).wait_send()
    for g in range(2):
        give_s(g).wait_send()


def finish_layer(*operands):
    block = GROUP * ROWS
    return pl.pallas_call(
        mlp_kernel,
        in_specs=[ANY] * 5 + [VMEM] + [ANY] * 7,
        out_specs=VMEM,
        out_shape=jax.ShapeDtypeStruct((REQ, ROWS, WIDTH), jnp.bfloat16),
        scratch_shapes=[
            pltpu.VMEM((2, REQ, ROWS, WIDTH), jnp.bfloat16),
            pltpu.VMEM((2, REQ, ROWS, WIDTH), jnp.bfloat16),
            pltpu.VMEM((WIDTH, WIDTH), jnp.bfloat16),
            pltpu.VMEM((FFN_PAD, WIDTH), jnp.bfloat16),
            pltpu.VMEM((FFN_PAD, WIDTH), jnp.bfloat16),
            pltpu.VMEM((FFN_PAD, WIDTH), jnp.bfloat16),
            pltpu.VMEM((4, 2, block, WIDTH), jnp.bfloat16),
            pltpu.VMEM((2 * block, FFN_PAD), jnp.bfloat16),
            pltpu.VMEM((4, block, WIDTH), jnp.bfloat16),
            pltpu.VMEM((4, block, WIDTH), jnp.bfloat16),
            pltpu.VMEM((4, block, WIDTH), jnp.float32),
            pltpu.VMEM((2, block, WIDTH), jnp.bfloat16),
            pltpu.VMEM((2, block, WIDTH), jnp.bfloat16),
            pltpu.VMEM((2, block, WIDTH), jnp.bfloat16),
            DMA((3,)), DMA((4,)), DMA((3,)),
            DMA((2, 2, 3)), DMA((2, 2, 3)), DMA((2, 2)),
            DMA, DMA, DMA((5,)), DMA((5,)),
            DMA((4,)), DMA((4,)), DMA((4,)), DMA((4,)), DMA((2,)), DMA((2,)),
        ],
        compiler_params=pltpu.CompilerParams(collective_id=1, has_side_effects=True, vmem_limit_bytes=62 * 1024 * 1024),
        name="finish_layer",
    )(*operands)


def solution(mesh):
    row_spec = P("dp", "tp", None)
    cache_spec = P("dp", None, "tp", None)
    req_spec = P("dp")
    rep_spec = P(None)
    col_spec = P(None, "tp")
    bias_spec = P("tp")
    down_spec = P("tp", None)

    def layer(x_rows, k_cache, v_cache, prefix, valid, g_attn, w_q, b_q, w_k, b_k, w_v, b_v, w_o, g_mlp, w_gate, w_up, w_down):
        cache_shape = (REQ, k_cache.shape[1], HEAD)
        k_old, v_old = k_cache.reshape(cache_shape), v_cache.reshape(cache_shape)
        across_chips = [(0, 2), (1, 3), (2, 0), (3, 1)]
        shared = (g_attn, b_q, b_k, b_v) + rope_tables()
        weights = (w_q, w_k, w_v)
        *first, pair0, wo_first, wo_rest = project_first(prefix, x_rows, shared, weights, w_o)
        mine, far0 = first[:3], first[3:]
        x_late, far0[0] = lax.optimization_barrier((x_rows[HALF_REQ:], far0[0]))
        pair1 = lax.ppermute(x_late, "tp", across_chips)
        o0, k_out, v_out = attention(0, prefix, valid, mine, far0, k_old, v_old)
        wo_first, pair1, k_out = lax.optimization_barrier((wo_first, pair1, k_out))
        near0 = lax.ppermute(wo_first, "tp", across_chips)
        far1 = list(project_second(prefix, pair1, shared, weights))
        near0, wo_rest, far1[0] = lax.optimization_barrier((near0, wo_rest, far1[0]))
        across0 = lax.ppermute(near0, "dp", [(0, 1), (1, 0)])
        near1 = lax.ppermute(wo_rest, "tp", across_chips)
        o1, k_out, v_out = attention(HALF_REQ, prefix, valid, mine, far1, k_old, v_old, (k_out, v_out))
        blocks = (HALF_REQ, 4, ROWS, 3 * HEAD)
        x_out = finish_layer(o0.reshape(blocks), o1.reshape(blocks), x_rows, pair0, pair1, g_mlp, w_o, near0, across0, near1, w_gate.T, w_up.T, w_down)
        return x_out, k_out.reshape(k_cache.shape), v_out.reshape(v_cache.shape)

    in_specs = (row_spec, cache_spec, cache_spec, req_spec, req_spec, rep_spec, col_spec, bias_spec, col_spec, bias_spec, col_spec, bias_spec, down_spec, rep_spec, col_spec, col_spec, down_spec)
    return jax.shard_map(layer, mesh=mesh, in_specs=in_specs, out_specs=(row_spec, cache_spec, cache_spec), check_vma=False)
```

```python
import jax
import jax.numpy as jnp
import numpy as np
from jax import lax
from jax.experimental import pallas as pl
from jax.experimental.pallas import tpu as pltpu
from jax.sharding import PartitionSpec as P

ROPE_THETA = 1.0e6
NORM_EPS = 1.0e-6
LOG2E = 1.4426950408889634
MESH = pl.DeviceIdType.MESH
ANY = pl.BlockSpec(memory_space=pl.ANY)
VMEM = pl.BlockSpec(memory_space=pltpu.VMEM)
SMEM = pl.BlockSpec(memory_space=pltpu.SMEM)
DMA = pltpu.SemaphoreType.DMA
REQ = 6
ROWS = 64
WIDTH = 1536
HEAD = 128
FFN = 2240
FFN_PAD = 2304
FFN_TILE = 768
GROUP = 3
HALF_WIDTH = 768


def rms_norm(wide, gain):
    inv_rms = lax.rsqrt(jnp.mean(wide * wide, axis=-1, keepdims=True) + NORM_EPS)
    return (wide * inv_rms * gain).astype(jnp.bfloat16)


def partners():
    me = lax.axis_index("tp")
    chip, core = me // 2, me % 2
    return lax.axis_index("dp"), (me, chip * 2 + 1 - core, (1 - chip) * 2 + core, (1 - chip) * 2 + 1 - core)


def greet(devices):
    barrier = pltpu.get_barrier_semaphore()
    for device in devices:
        pl.semaphore_signal(barrier, inc=1, device_id=device, device_id_type=MESH)
    pl.semaphore_wait(barrier, len(devices))


def send(src, dst, send_sem, recv_sem, device):
    return pltpu.make_async_remote_copy(src_ref=src, dst_ref=dst, send_sem=send_sem, recv_sem=recv_sem, device_id=device, device_id_type=MESH)


def rope_tables():
    freq = ROPE_THETA ** (-(np.arange(HEAD // 2, dtype=np.float64) * 2.0) / HEAD)
    freq = np.concatenate([freq, freq])
    angles = np.arange(4 * ROWS, dtype=np.float64)[:, None] * freq
    return np.cos(angles).astype(np.float32), np.sin(angles).astype(np.float32), freq.astype(np.float32)[None]


def load_shared(refs, bufs, sem):
    gain, bq, bk, bv, cos, sin, freq, wq, wk, wv = refs
    small, wbuf = bufs[:7], bufs[7]
    pairs = list(zip((gain, bq, bk, bv, cos, sin, freq), small))
    pairs += [(wq, wbuf.at[:, pl.ds(0, 384)]), (wk, wbuf.at[:, pl.ds(384, 128)]), (wv, wbuf.at[:, pl.ds(512, 128)])]
    return [pltpu.make_async_copy(src, dst, sem.at[i]) for i, (src, dst) in enumerate(pairs)]


SHARED_SCRATCH = [
    pltpu.VMEM((WIDTH,), jnp.bfloat16), pltpu.VMEM((384,), jnp.bfloat16), pltpu.VMEM((128,), jnp.bfloat16), pltpu.VMEM((128,), jnp.bfloat16),
    pltpu.VMEM((4 * ROWS, HEAD), jnp.float32), pltpu.VMEM((4 * ROWS, HEAD), jnp.float32), pltpu.VMEM((1, HEAD), jnp.float32),
    pltpu.VMEM((WIDTH, 640), jnp.bfloat16), DMA((10,)),
]


def qkv_scratch(n_req):
    return [
        pltpu.VMEM((n_req, 3, 2 * ROWS, HEAD), jnp.bfloat16),
        pltpu.VMEM((n_req, 2 * ROWS, HEAD), jnp.bfloat16),
        pltpu.VMEM((n_req, 2 * ROWS, HEAD), jnp.bfloat16),
        DMA((3, n_req)),
    ]


def give_qkv(bufs, refs, sem, r):
    return [pltpu.make_async_copy(buf.at[r], ref.at[r], sem.at[i, r]) for i, (buf, ref) in enumerate(zip(bufs, refs))]


def project(x, position, chip, shared, outs, r):
    g_ref, *biases, cos_ref, sin_ref, freq_ref, wbuf = shared
    q_ref, k_ref, v_ref = outs
    rows = pl.ds(pl.multiple_of(chip * 2 * ROWS, 2 * ROWS), 2 * ROWS)
    normed = rms_norm(x.astype(jnp.float32), g_ref[...].astype(jnp.float32).reshape(1, WIDTH))
    total = jnp.dot(normed, wbuf[...], preferred_element_type=jnp.float32)
    angle = jnp.full((8, HEAD), position, jnp.int32).astype(jnp.float32) * freq_ref[...]
    cos_p, sin_p = jnp.cos(angle)[:1], jnp.sin(angle)[:1]
    cos_i, sin_i = cos_ref[rows, :], sin_ref[rows, :]
    cos_t = cos_p * cos_i - sin_p * sin_i
    sin_t = sin_p * cos_i + cos_p * sin_i
    lane = lax.broadcasted_iota(jnp.int32, sin_t.shape, 1)
    sin_t = jnp.where(lane < HEAD // 2, -sin_t, sin_t)
    bias = jnp.concatenate([b[...].astype(jnp.float32).reshape(1, b.shape[0]) for b in biases], axis=1)
    rounded = (total + bias).astype(jnp.bfloat16)
    for head in range(4):
        part = rounded[:, head * HEAD:(head + 1) * HEAD].astype(jnp.float32)
        turned = (part * cos_t + pltpu.roll(part, HEAD // 2, 1) * sin_t).astype(jnp.bfloat16)
        if head < 3:
            q_ref[r, head] = turned
        else:
            k_ref[r] = turned
    v_ref[r] = rounded[:, 4 * HEAD:]


def qkv_kernel(prefix_ref, x_ref, *refs):
    shared_refs, mine_refs, far_refs, pair_ref = refs[:10], refs[10:13], refs[13:16], refs[16]
    own, other = refs[17:19]
    shared, shared_sem = refs[19:27], refs[27]
    mine, mine_sem = refs[28:31], refs[31]
    far, far_sem = refs[32:35], refs[35]
    in_sem, out_sem, sx, rx, sc, rc, sf, rf = refs[36:]
    dp, (me, core_peer, chip_peer, _) = partners()
    chip, core = me // 2, me % 2
    load_x = pltpu.make_async_copy(x_ref, own.at[core], in_sem)
    load_x.start()
    loads = load_shared(shared_refs, shared, shared_sem)
    greet([(dp, core_peer), (dp, chip_peer)])
    load_x.wait()

    def to_chip(r):
        return send(own.at[core, r], other.at[core, r], sx.at[r], rx.at[r], (dp, chip_peer))

    def to_core(r):
        return send(own.at[core, r], own.at[core, r], sc.at[r], rc.at[r], (dp, core_peer))

    def forward(r):
        return send(other.at[core, r], other.at[core, r], sf.at[r], rf.at[r], (dp, core_peer))

    def keep(r):
        return pltpu.make_async_copy(other.at[core, r], pair_ref.at[r], out_sem.at[r])

    for r in range(REQ):
        to_chip(r).start()
    for r in range(REQ):
        to_core(r).start()
    for load in loads:
        load.start()
    for load in loads:
        load.wait()

    @pl.loop(0, REQ)
    def _(r):
        to_core(r).wait_recv()
        project(own[:, r].reshape(2 * ROWS, WIDTH), prefix_ref[r], chip, shared, mine, r)
        for copy in give_qkv(mine, mine_refs, mine_sem, r):
            copy.start()

    @pl.loop(0, REQ + 1)
    def _(r):
        @pl.when(r < REQ)
        def _():
            to_chip(r).wait_recv()
            forward(r).start()
            keep(r).start()

        @pl.when(r > 0)
        def _():
            forward(r - 1).wait_recv()
            project(other[:, r - 1].reshape(2 * ROWS, WIDTH), prefix_ref[r - 1], 1 - chip, shared, far, r - 1)
            for copy in give_qkv(far, far_refs, far_sem, r - 1):
                copy.start()

    @pl.loop(0, REQ)
    def _(r):
        to_core(r).wait_send()
        for copy in give_qkv(mine, mine_refs, mine_sem, r):
            copy.wait()
        to_chip(r).wait_send()
        forward(r).wait_send()
        keep(r).wait()
        for copy in give_qkv(far, far_refs, far_sem, r):
            copy.wait()


def qkv_shapes(n_req):
    return [
        jax.ShapeDtypeStruct((n_req, 3, 2 * ROWS, HEAD), jnp.bfloat16),
        jax.ShapeDtypeStruct((n_req, 2 * ROWS, HEAD), jnp.bfloat16),
        jax.ShapeDtypeStruct((n_req, 2 * ROWS, HEAD), jnp.bfloat16),
    ]


def project_rows(prefix, x_rows, shared):
    return pl.pallas_call(
        qkv_kernel,
        in_specs=[SMEM] + [ANY] * 11,
        out_specs=[ANY] * 7,
        out_shape=qkv_shapes(REQ) + qkv_shapes(REQ) + [jax.ShapeDtypeStruct((REQ, ROWS, WIDTH), jnp.bfloat16)],
        scratch_shapes=[
            pltpu.VMEM((2, REQ, ROWS, WIDTH), jnp.bfloat16),
            pltpu.VMEM((2, REQ, ROWS, WIDTH), jnp.bfloat16),
            *SHARED_SCRATCH, *qkv_scratch(REQ), *qkv_scratch(REQ),
            DMA, DMA((REQ,)), DMA((REQ,)), DMA((REQ,)), DMA((REQ,)), DMA((REQ,)), DMA((REQ,)), DMA((REQ,)),
        ],
        compiler_params=pltpu.CompilerParams(collective_id=0, has_side_effects=True),
        cost_estimate=pl.CostEstimate(flops=2 * 10 ** 9, bytes_accessed=60 * 10 ** 6, transcendentals=0),
        name="project_rows",
    )(prefix, x_rows, *shared)


BLOCK_KV = 512
WINDOW = 272


def attn_kernel(prefix_ref, valid_ref, qa_ref, ka_ref, va_ref, qb_ref, kb_ref, vb_ref, k_ref, v_ref, *refs):
    o_ref, ko_ref, vo_ref, kbuf, vbuf, obuf, qa, ka, va, qb, kb, vb, qbuf, fbuf, acc_ref, m_ref, l_ref, even_ref, odd_ref, k_sem, v_sem, out_sem, in_sem = refs
    n_req, heads = REQ, 3
    rows, dim = 4 * ROWS, HEAD
    slots = kbuf.shape[1]
    chip = lax.axis_index("tp") // 2
    ours = pl.ds(pl.multiple_of(chip * 2 * ROWS, 2 * ROWS), 2 * ROWS)
    theirs = pl.ds(pl.multiple_of((1 - chip) * 2 * ROWS, 2 * ROWS), 2 * ROWS)
    last = slots // BLOCK_KV - 1
    factor = (dim ** -0.5) * LOG2E

    def copies(r):
        return (
            (pltpu.make_async_copy(k_ref.at[r], kbuf.at[r], k_sem.at[r]), pltpu.make_async_copy(v_ref.at[r], vbuf.at[r], v_sem.at[r])),
            (pltpu.make_async_copy(kbuf.at[r], ko_ref.at[r], out_sem.at[0, r]), pltpu.make_async_copy(vbuf.at[r], vo_ref.at[r], out_sem.at[1, r])),
            pltpu.make_async_copy(obuf.at[r], o_ref.at[r], out_sem.at[2, r]),
        )

    news = (
        pltpu.make_async_copy(ka_ref, ka, in_sem.at[0]),
        pltpu.make_async_copy(kb_ref, kb, in_sem.at[1]),
        pltpu.make_async_copy(va_ref, va, in_sem.at[2]),
        pltpu.make_async_copy(vb_ref, vb, in_sem.at[3]),
        pltpu.make_async_copy(qa_ref, qa, in_sem.at[4]),
        pltpu.make_async_copy(qb_ref, qb, in_sem.at[5]),
    )

    def merge(mine, far, buf, r, start, count):
        base = pl.multiple_of(jnp.minimum((start // 16) * 16, slots - WINDOW), 16)
        shift = start - base
        fbuf[ours, :] = mine.astype(jnp.float32)
        fbuf[theirs, :] = far.astype(jnp.float32)
        rolled = pltpu.roll(fbuf[...], shift, 0)
        idx = lax.broadcasted_iota(jnp.int32, rolled.shape, 0) - shift
        window = buf[r, pl.ds(base, WINDOW), :].astype(jnp.float32)
        merged = jnp.where((idx >= 0) & (idx < count), rolled, window)
        buf[r, pl.ds(base, WINDOW), :] = merged.astype(jnp.bfloat16)

    for copy in news:
        copy.start()
    for load in copies(0)[0]:
        load.start()
    fbuf[rows:, :] = jnp.zeros((WINDOW - rows, dim), jnp.float32)
    for copy in news:
        copy.wait()

    @pl.loop(0, n_req)
    def _(r):
        start = prefix_ref[r]
        count = valid_ref[r]
        loads, stores, give = copies(r)
        for load in loads:
            load.wait()

        @pl.when(r + 1 < n_req)
        def _():
            for load in copies(r + 1)[0]:
                load.start()

        merge(ka[r], kb[r], kbuf, r, start, count)
        merge(va[r], vb[r], vbuf, r, start, count)
        for store in stores:
            store.start()
        acc_ref[...] = jnp.zeros_like(acc_ref)
        l_ref[...] = jnp.zeros_like(l_ref)
        m_ref[...] = jnp.full_like(m_ref, -1.0e30)
        n_full = start // BLOCK_KV
        n_all = (start + count + BLOCK_KV - 1) // BLOCK_KV
        for h in range(heads):
            qbuf[h, ours, :] = qa[r, h]
            qbuf[h, theirs, :] = qb[r, h]
        wide = qbuf[...].reshape(heads * rows, dim).astype(jnp.float32) * factor
        high = wide.astype(jnp.bfloat16)
        low = (wide - high.astype(jnp.float32)).astype(jnp.bfloat16)
        queries = jnp.concatenate([high, low], axis=1)

        def scores(blk, dst):
            off = pl.multiple_of(jnp.minimum(blk, last) * BLOCK_KV, BLOCK_KV)
            keys = kbuf[r, pl.ds(off, BLOCK_KV), :]
            keys = jnp.concatenate([keys, keys], axis=1)
            s = lax.dot_general(queries, keys, (((1,), (1,)), ((), ())), preferred_element_type=jnp.float32)
            dst[...] = s

        def absorb(blk, src, masked):
            off = pl.multiple_of(blk * BLOCK_KV, BLOCK_KV)
            vals = vbuf[r, pl.ds(off, BLOCK_KV), :]
            s = src[...]
            if masked:
                row = lax.broadcasted_iota(jnp.int32, (rows, BLOCK_KV), 0)
                col = lax.broadcasted_iota(jnp.int32, (rows, BLOCK_KV), 1)
                visible = col + off <= start + jnp.minimum(row, count - 1)
                s = jnp.where(jnp.concatenate([visible] * heads, axis=0), s, -1.0e30)
            m_old = m_ref[...]
            best = jnp.max(s, axis=1, keepdims=True)
            m_new = jnp.maximum(m_old, best)
            alpha = jnp.exp2(m_old - m_new)
            p = jnp.exp2(s - m_new[:, :1])
            part = p[:, :128]
            for j in range(1, BLOCK_KV // 128):
                part = part + p[:, j * 128:(j + 1) * 128]
            l_ref[...] = l_ref[...] * alpha + part
            m_ref[...] = m_new
            acc_ref[...] = acc_ref[...] * alpha + jnp.dot(p.astype(jnp.bfloat16), vals, preferred_element_type=jnp.float32)

        def step(blk, masked):
            @pl.when(blk % 2 == 0)
            def _():
                scores(blk + 1, odd_ref)
                absorb(blk, even_ref, masked)

            @pl.when(blk % 2 == 1)
            def _():
                scores(blk + 1, even_ref)
                absorb(blk, odd_ref, masked)

        scores(0, even_ref)

        @pl.loop(0, n_full)
        def _(blk):
            step(blk, False)

        @pl.loop(n_full, n_all)
        def _(blk):
            step(blk, True)

        for h in range(heads):
            at = slice(h * rows, (h + 1) * rows)
            total = jnp.sum(l_ref[at], axis=1, keepdims=True)
            obuf[r, :, h * dim:(h + 1) * dim] = (acc_ref[at] / total).astype(jnp.bfloat16)
        give.start()

    @pl.loop(0, n_req)
    def _(r):
        _, stores, give = copies(r)
        for store in stores:
            store.wait()
        give.wait()


def attention(prefix, valid, mine, far, k_cache, v_cache):
    part = (REQ, 2 * ROWS, HEAD)
    state = pltpu.VMEM((3 * 4 * ROWS, HEAD), jnp.float32)
    tile = pltpu.VMEM((3 * 4 * ROWS, BLOCK_KV), jnp.float32)
    slots = pltpu.VMEM((REQ,) + k_cache.shape[1:], jnp.bfloat16)
    q_part = pltpu.VMEM((REQ, 3, 2 * ROWS, HEAD), jnp.bfloat16)
    kv_part = pltpu.VMEM(part, jnp.bfloat16)
    return pl.pallas_call(
        attn_kernel,
        in_specs=[SMEM, SMEM] + [ANY] * 8,
        out_specs=[ANY, ANY, ANY],
        scratch_shapes=[
            slots, slots, pltpu.VMEM((REQ, 4 * ROWS, 3 * HEAD), jnp.bfloat16),
            q_part, kv_part, kv_part, q_part, kv_part, kv_part,
            pltpu.VMEM((3, 4 * ROWS, HEAD), jnp.bfloat16),
            pltpu.VMEM((WINDOW, HEAD), jnp.float32),
            state, state, state, tile, tile,
            DMA((REQ,)), DMA((REQ,)), DMA((3, REQ)), DMA((6,)),
        ],
        out_shape=[
            jax.ShapeDtypeStruct((REQ, 4 * ROWS, 3 * HEAD), jnp.bfloat16),
            jax.ShapeDtypeStruct(k_cache.shape, jnp.bfloat16),
            jax.ShapeDtypeStruct(v_cache.shape, jnp.bfloat16),
        ],
        cost_estimate=pl.CostEstimate(flops=10 ** 10, bytes_accessed=40 * 10 ** 6, transcendentals=7 * 10 ** 6),
        name="attention",
    )(prefix, valid, *mine, *far, k_cache, v_cache)


def mlp_kernel(o_ref, x_ref, pair_ref, g_ref, wo_ref, far_ref, wg_ref, wu_ref, wd_ref, out_ref,
               osrc, obuf, xin, wo, wg, wu, wd, hbuf, ubuf, psend, precv, pown, xsend, xrecv, x1buf, outbuf,
               w_sem, wl_sem, in_sem, o_sem, so, ro, lo, swc, rwc, sh, rh, sp, rp, ss, rs):
    dp, peers = partners()
    me, core_peer, chip_peer, far_peer = peers

    def cols(who):
        return pl.ds(pl.multiple_of(who * 384, 384), 384)

    def share(slot, g, s):
        block = peers[s] if slot == 0 else peers[s ^ 2]
        src = (o_ref if s == 0 else osrc).at[pl.ds(GROUP * g, GROUP), block]
        dst = obuf.at[slot, pl.ds(GROUP * g, GROUP), :, cols(me)]
        if s == 0:
            return pltpu.make_async_copy(src, dst, lo.at[slot, g])
        return send(src, dst, so.at[slot, g, s - 1], ro.at[slot, g, s - 1], (dp, peers[s]))

    have = tuple((src, wo.at[pl.ds(pl.multiple_of(who * 384, 384), 384)]) for src, who in ((wo_ref, me), (far_ref, chip_peer)))
    wo_local = tuple(pltpu.make_async_copy(src, dst, wl_sem.at[i]) for i, (src, dst) in enumerate(have))
    wo_core = tuple(send(src, dst, swc.at[i], rwc.at[i], (dp, core_peer)) for i, (src, dst) in enumerate(have))
    weights = (
        pltpu.make_async_copy(wg_ref, wg.at[pl.ds(0, FFN)], w_sem.at[0]),
        pltpu.make_async_copy(wu_ref, wu.at[pl.ds(0, FFN)], w_sem.at[1]),
        pltpu.make_async_copy(wd_ref, wd.at[pl.ds(0, FFN)], w_sem.at[2]),
    )
    x_loads = (
        pltpu.make_async_copy(x_ref, xin.at[0], in_sem.at[0]),
        pltpu.make_async_copy(pair_ref, xin.at[1], in_sem.at[1]),
    )
    order = ((1, 0), (1, 1), (0, 0), (0, 1))

    load_o = pltpu.make_async_copy(o_ref, osrc, in_sem.at[2])
    load_o.start()
    for copy in wo_local + x_loads:
        copy.start()
    greet([(dp, core_peer), (dp, chip_peer), (dp, far_peer)])
    load_o.wait()
    for slot, g in order:
        for s in (2, 3, 1):
            share(slot, g, s).start()
    for copy in wo_core:
        copy.start()
    for slot, g in order:
        share(slot, g, 0).start()
    pad = jnp.zeros((FFN_PAD - FFN, WIDTH), jnp.bfloat16)
    for buf in (wg, wu, wd):
        buf[FFN:, :] = pad

    gain = g_ref[...].astype(jnp.float32).reshape(1, WIDTH)

    def give_h(k):
        return send(hbuf.at[k, 0], hbuf.at[k, 1], sh.at[k], rh.at[k], (dp, core_peer))

    def part(n):
        return pl.ds(pl.multiple_of(n * HALF_WIDTH, HALF_WIDTH), HALF_WIDTH)

    def give_p(k, n):
        return send(psend.at[k, :, part(n)], precv.at[k, :, part(n)], sp.at[k, n], rp.at[k, n], (dp, core_peer))

    def give_s(g, n):
        return send(xsend.at[g, :, part(n)], xrecv.at[g, :, part(n)], ss.at[g, n], rs.at[g, n], (dp, chip_peer))

    def give_out(g, n):
        reqs = pl.ds(GROUP * g, GROUP)
        return pltpu.make_async_copy(outbuf.at[reqs, :, part(n)], out_ref.at[reqs, :, part(n)], o_sem.at[g, n])

    def attn_out(k):
        slot, g = order[k]
        for s in (2, 3, 1):
            share(slot, g, s).wait_recv()
        share(slot, g, 0).wait()
        reqs = slice(GROUP * g, GROUP * (g + 1))
        heads = obuf[slot, reqs].reshape(GROUP * ROWS, WIDTH)
        attn = jnp.dot(heads, wo[...], preferred_element_type=jnp.float32).astype(jnp.bfloat16)
        base = xin[slot, reqs].reshape(GROUP * ROWS, WIDTH)
        mid = (base.astype(jnp.float32) + attn.astype(jnp.float32)).astype(jnp.bfloat16)
        if slot == 0:
            x1buf[g] = mid
        hbuf[k, 0] = rms_norm(mid.astype(jnp.float32), gain)
        give_h(k).start()

    def mlp(k):
        give_h(k).wait_recv()
        if k == 0:
            weights[0].wait()
            weights[1].wait()
        hidden = hbuf.at[k].reshape(2 * GROUP * ROWS, WIDTH)

        @pl.loop(0, FFN_PAD // FFN_TILE)
        def _(f):
            at = pl.ds(pl.multiple_of(f * FFN_TILE, FFN_TILE), FFN_TILE)
            nt = (((1,), (1,)), ((), ()))
            gate = lax.dot_general(hidden[...], wg[at, :], nt, preferred_element_type=jnp.float32)
            up = lax.dot_general(hidden[...], wu[at, :], nt, preferred_element_type=jnp.float32)
            ubuf[:, at] = (jax.nn.silu(gate) * up).astype(jnp.bfloat16)

        if k == 0:
            weights[2].wait()

        @pl.loop(0, 2)
        def _(n):
            down = jnp.dot(ubuf[...], wd[:, part(n)], preferred_element_type=jnp.float32)
            pown[k, :, part(n)] = down[:GROUP * ROWS]
            psend[k, :, part(n)] = down[GROUP * ROWS:].astype(jnp.bfloat16)
            give_p(k, n).start()

    def combine(k):
        slot, g = order[k]

        @pl.loop(0, 2)
        def _(n):
            give_p(k, n).wait_recv()
            total = pown[k, :, part(n)] + precv[k, :, part(n)].astype(jnp.float32)
            if slot == 1:
                xsend[g, :, part(n)] = total.astype(jnp.bfloat16)
                give_s(g, n).start()
            else:
                give_s(g, n).wait_recv()
                down = (total + xrecv[g, :, part(n)].astype(jnp.float32)).astype(jnp.bfloat16)
                out = (x1buf[g, :, part(n)].astype(jnp.float32) + down.astype(jnp.float32)).astype(jnp.bfloat16)
                outbuf[GROUP * g:GROUP * (g + 1), :, part(n)] = out.reshape(GROUP, ROWS, HALF_WIDTH)
                give_out(g, n).start()

    for copy in wo_local + x_loads:
        copy.wait()
    for copy in weights:
        copy.start()
    for copy in wo_core:
        copy.wait_recv()
    attn_out(0)
    mlp(0)
    attn_out(1)
    attn_out(2)
    combine(0)
    mlp(1)
    attn_out(3)
    combine(1)
    mlp(2)
    combine(2)
    mlp(3)
    combine(3)
    for copy in wo_core:
        copy.wait_send()
    for k, (slot, g) in enumerate(order):
        for s in (2, 3, 1):
            share(slot, g, s).wait_send()
        give_h(k).wait_send()
        for n in range(2):
            give_p(k, n).wait_send()
    for g in range(2):
        for n in range(2):
            give_s(g, n).wait_send()
            give_out(g, n).wait()


def finish_layer(*operands):
    block = GROUP * ROWS
    return pl.pallas_call(
        mlp_kernel,
        in_specs=[ANY] * 3 + [VMEM] + [ANY] * 5,
        out_specs=ANY,
        out_shape=jax.ShapeDtypeStruct((REQ, ROWS, WIDTH), jnp.bfloat16),
        scratch_shapes=[
            pltpu.VMEM((REQ, 4, ROWS, 3 * HEAD), jnp.bfloat16),
            pltpu.VMEM((2, REQ, ROWS, WIDTH), jnp.bfloat16),
            pltpu.VMEM((2, REQ, ROWS, WIDTH), jnp.bfloat16),
            pltpu.VMEM((WIDTH, WIDTH), jnp.bfloat16),
            pltpu.VMEM((FFN_PAD, WIDTH), jnp.bfloat16),
            pltpu.VMEM((FFN_PAD, WIDTH), jnp.bfloat16),
            pltpu.VMEM((FFN_PAD, WIDTH), jnp.bfloat16),
            pltpu.VMEM((4, 2, block, WIDTH), jnp.bfloat16),
            pltpu.VMEM((2 * block, FFN_PAD), jnp.bfloat16),
            pltpu.VMEM((4, block, WIDTH), jnp.bfloat16),
            pltpu.VMEM((4, block, WIDTH), jnp.bfloat16),
            pltpu.VMEM((4, block, WIDTH), jnp.float32),
            pltpu.VMEM((2, block, WIDTH), jnp.bfloat16),
            pltpu.VMEM((2, block, WIDTH), jnp.bfloat16),
            pltpu.VMEM((2, block, WIDTH), jnp.bfloat16),
            pltpu.VMEM((REQ, ROWS, WIDTH), jnp.bfloat16),
            DMA((3,)), DMA((2,)), DMA((3,)), DMA((2, 2)),
            DMA((2, 2, 3)), DMA((2, 2, 3)), DMA((2, 2)),
            DMA((2,)), DMA((2,)),
            DMA((4,)), DMA((4,)), DMA((4, 2)), DMA((4, 2)), DMA((2, 2)), DMA((2, 2)),
        ],
        compiler_params=pltpu.CompilerParams(collective_id=1, has_side_effects=True, vmem_limit_bytes=62 * 1024 * 1024),
        name="finish_layer",
    )(*operands)


def solution(mesh):
    row_spec = P("dp", "tp", None)
    cache_spec = P("dp", None, "tp", None)
    req_spec = P("dp")
    rep_spec = P(None)
    col_spec = P(None, "tp")
    bias_spec = P("tp")
    down_spec = P("tp", None)

    def layer(x_rows, k_cache, v_cache, prefix, valid, g_attn, w_q, b_q, w_k, b_k, w_v, b_v, w_o, g_mlp, w_gate, w_up, w_down):
        cache_shape = (REQ, k_cache.shape[1], HEAD)
        k_old, v_old = k_cache.reshape(cache_shape), v_cache.reshape(cache_shape)
        across_chips = [(0, 2), (1, 3), (2, 0), (3, 1)]
        shared = (g_attn, b_q, b_k, b_v) + rope_tables() + (w_q, w_k, w_v)
        *qkv, x_pair = project_rows(prefix, x_rows, shared)
        mine, far = qkv[:3], qkv[3:]
        w_own, far[0] = lax.optimization_barrier((w_o, far[0]))
        w_far = lax.ppermute(w_own, "tp", across_chips)
        o, k_out, v_out = attention(prefix, valid, mine, far, k_old, v_old)
        x_out = finish_layer(o.reshape(REQ, 4, ROWS, 3 * HEAD), x_rows, x_pair, g_mlp, w_o, w_far, w_gate.T, w_up.T, w_down)
        return x_out, k_out.reshape(k_cache.shape), v_out.reshape(v_cache.shape)

    in_specs = (row_spec, cache_spec, cache_spec, req_spec, req_spec, rep_spec, col_spec, bias_spec, col_spec, bias_spec, col_spec, bias_spec, down_spec, rep_spec, col_spec, col_spec, down_spec)
    return jax.shard_map(layer, mesh=mesh, in_specs=in_specs, out_specs=(row_spec, cache_spec, cache_spec), check_vma=False)
```

```python
import jax
import jax.numpy as jnp
import numpy as np
from jax import lax
from jax.experimental import pallas as pl
from jax.experimental.pallas import tpu as pltpu
from jax.sharding import PartitionSpec as P

ROPE_THETA = 1.0e6
NORM_EPS = 1.0e-6
LOG2E = 1.4426950408889634
MESH = pl.DeviceIdType.MESH
ANY = pl.BlockSpec(memory_space=pl.ANY)
VMEM = pl.BlockSpec(memory_space=pltpu.VMEM)
SMEM = pl.BlockSpec(memory_space=pltpu.SMEM)
DMA = pltpu.SemaphoreType.DMA
REQ = 6
ROWS = 64
WIDTH = 1536
HEAD = 128
FFN = 2240
FFN_PAD = 2304
FFN_TILE = 768
WO_EARLY = 32
STEPS = ((1, 0, 2), (1, 2, 2), (1, 4, 2), (0, 0, 3), (0, 3, 3))
STEP_ROWS = [ROWS * sum(n for _, _, n in STEPS[:k]) for k in range(len(STEPS))]
RS_NEED = {3: (0, 1), 4: (2,)}
ALL_ROWS = 2 * REQ * ROWS
MAX_ROWS = 2 * ROWS * max(n for _, _, n in STEPS)
HALF_WIDTH = 768


def rms_norm(wide, gain):
    inv_rms = lax.rsqrt(jnp.mean(wide * wide, axis=-1, keepdims=True) + NORM_EPS)
    return (wide * inv_rms * gain).astype(jnp.bfloat16)


def partners():
    me = lax.axis_index("tp")
    chip, core = me // 2, me % 2
    return lax.axis_index("dp"), (me, chip * 2 + 1 - core, (1 - chip) * 2 + core, (1 - chip) * 2 + 1 - core)


def greet(devices):
    barrier = pltpu.get_barrier_semaphore()
    for device in devices:
        pl.semaphore_signal(barrier, inc=1, device_id=device, device_id_type=MESH)
    pl.semaphore_wait(barrier, len(devices))


def send(src, dst, send_sem, recv_sem, device):
    return pltpu.make_async_remote_copy(src_ref=src, dst_ref=dst, send_sem=send_sem, recv_sem=recv_sem, device_id=device, device_id_type=MESH)


def rope_tables():
    freq = ROPE_THETA ** (-(np.arange(HEAD // 2, dtype=np.float64) * 2.0) / HEAD)
    freq = np.concatenate([freq, freq])
    angles = np.arange(4 * ROWS, dtype=np.float64)[:, None] * freq
    return np.cos(angles).astype(np.float32), np.sin(angles).astype(np.float32), freq.astype(np.float32)[None]


def load_shared(refs, bufs, sem):
    gain, bq, bk, bv, cos, sin, freq, wq, wk, wv = refs
    small, wbuf = bufs[:7], bufs[7]
    pairs = list(zip((gain, bq, bk, bv, cos, sin, freq), small))
    pairs += [(wq, wbuf.at[:, pl.ds(0, 384)]), (wk, wbuf.at[:, pl.ds(384, 128)]), (wv, wbuf.at[:, pl.ds(512, 128)])]
    return [pltpu.make_async_copy(src, dst, sem.at[i]) for i, (src, dst) in enumerate(pairs)]


SHARED_SCRATCH = [
    pltpu.VMEM((WIDTH,), jnp.bfloat16), pltpu.VMEM((384,), jnp.bfloat16), pltpu.VMEM((128,), jnp.bfloat16), pltpu.VMEM((128,), jnp.bfloat16),
    pltpu.VMEM((4 * ROWS, HEAD), jnp.float32), pltpu.VMEM((4 * ROWS, HEAD), jnp.float32), pltpu.VMEM((1, HEAD), jnp.float32),
    pltpu.VMEM((WIDTH, 640), jnp.bfloat16), DMA((10,)),
]


def qkv_scratch(n_req):
    return [
        pltpu.VMEM((n_req, 3, 2 * ROWS, HEAD), jnp.bfloat16),
        pltpu.VMEM((n_req, 2 * ROWS, HEAD), jnp.bfloat16),
        pltpu.VMEM((n_req, 2 * ROWS, HEAD), jnp.bfloat16),
        DMA((3, n_req)),
    ]


def give_qkv(bufs, refs, sem, r):
    return [pltpu.make_async_copy(buf.at[r], ref.at[r], sem.at[i, r]) for i, (buf, ref) in enumerate(zip(bufs, refs))]


def project(x, position, chip, shared, outs, r):
    g_ref, *biases, cos_ref, sin_ref, freq_ref, wbuf = shared
    q_ref, k_ref, v_ref = outs
    rows = pl.ds(pl.multiple_of(chip * 2 * ROWS, 2 * ROWS), 2 * ROWS)
    normed = rms_norm(x.astype(jnp.float32), g_ref[...].astype(jnp.float32).reshape(1, WIDTH))
    total = jnp.dot(normed, wbuf[...], preferred_element_type=jnp.float32)
    angle = jnp.full((8, HEAD), position, jnp.int32).astype(jnp.float32) * freq_ref[...]
    cos_p, sin_p = jnp.cos(angle)[:1], jnp.sin(angle)[:1]
    cos_i, sin_i = cos_ref[rows, :], sin_ref[rows, :]
    cos_t = cos_p * cos_i - sin_p * sin_i
    sin_t = sin_p * cos_i + cos_p * sin_i
    lane = lax.broadcasted_iota(jnp.int32, sin_t.shape, 1)
    sin_t = jnp.where(lane < HEAD // 2, -sin_t, sin_t)
    bias = jnp.concatenate([b[...].astype(jnp.float32).reshape(1, b.shape[0]) for b in biases], axis=1)
    rounded = (total + bias).astype(jnp.bfloat16)
    for head in range(4):
        part = rounded[:, head * HEAD:(head + 1) * HEAD].astype(jnp.float32)
        turned = (part * cos_t + pltpu.roll(part, HEAD // 2, 1) * sin_t).astype(jnp.bfloat16)
        if head < 3:
            q_ref[r, head] = turned
        else:
            k_ref[r] = turned
    v_ref[r] = rounded[:, 4 * HEAD:]


def qkv_kernel(prefix_ref, x_ref, *refs):
    shared_refs, wo_ref, mine_refs, far_refs, pair_ref, early_ref = refs[:10], refs[10], refs[11:14], refs[14:17], refs[17], refs[18]
    late_ref, own, other, late = refs[19:23]
    shared, shared_sem = refs[23:31], refs[31]
    mine, mine_sem = refs[32:35], refs[35]
    far, far_sem = refs[36:39], refs[39]
    in_sem, out_sem, sx, rx, sc, rc, sf, rf, se, re, late_sem = refs[40:]
    dp, (me, core_peer, chip_peer, _) = partners()
    chip, core = me // 2, me % 2
    load_x = pltpu.make_async_copy(x_ref, own.at[core], in_sem)
    load_x.start()
    loads = load_shared(shared_refs, shared, shared_sem)
    greet([(dp, core_peer), (dp, chip_peer)])
    load_x.wait()

    def to_chip(r):
        return send(own.at[core, r], other.at[core, r], sx.at[r], rx.at[r], (dp, chip_peer))

    def to_core(r):
        return send(own.at[core, r], own.at[core, r], sc.at[r], rc.at[r], (dp, core_peer))

    def forward(r):
        return send(other.at[core, r], other.at[core, r], sf.at[r], rf.at[r], (dp, core_peer))

    def keep(r):
        return pltpu.make_async_copy(other.at[core, r], pair_ref.at[r], out_sem.at[r])

    early = send(wo_ref.at[pl.ds(0, WO_EARLY)], early_ref, se, re, (dp, chip_peer))
    for r in range(REQ):
        to_chip(r).start()
    early.start()
    for r in range(REQ):
        to_core(r).start()
    take_late = pltpu.make_async_copy(wo_ref.at[pl.ds(WO_EARLY, 384 - WO_EARLY)], late, late_sem.at[0])
    give_late = pltpu.make_async_copy(late, late_ref, late_sem.at[1])
    for load in loads:
        load.start()
    take_late.start()
    for load in loads:
        load.wait()
    take_late.wait()
    give_late.start()

    @pl.loop(0, REQ)
    def _(r):
        to_core(r).wait_recv()
        project(own[:, r].reshape(2 * ROWS, WIDTH), prefix_ref[r], chip, shared, mine, r)
        for copy in give_qkv(mine, mine_refs, mine_sem, r):
            copy.start()

    @pl.loop(0, REQ + 1)
    def _(r):
        @pl.when(r < REQ)
        def _():
            to_chip(r).wait_recv()
            forward(r).start()
            keep(r).start()

        @pl.when(r > 0)
        def _():
            forward(r - 1).wait_recv()
            project(other[:, r - 1].reshape(2 * ROWS, WIDTH), prefix_ref[r - 1], 1 - chip, shared, far, r - 1)
            for copy in give_qkv(far, far_refs, far_sem, r - 1):
                copy.start()

    early.wait()
    give_late.wait()

    @pl.loop(0, REQ)
    def _(r):
        to_core(r).wait_send()
        for copy in give_qkv(mine, mine_refs, mine_sem, r):
            copy.wait()
        to_chip(r).wait_send()
        forward(r).wait_send()
        keep(r).wait()
        for copy in give_qkv(far, far_refs, far_sem, r):
            copy.wait()


def qkv_shapes(n_req):
    return [
        jax.ShapeDtypeStruct((n_req, 3, 2 * ROWS, HEAD), jnp.bfloat16),
        jax.ShapeDtypeStruct((n_req, 2 * ROWS, HEAD), jnp.bfloat16),
        jax.ShapeDtypeStruct((n_req, 2 * ROWS, HEAD), jnp.bfloat16),
    ]


def project_rows(prefix, x_rows, shared, w_o):
    return pl.pallas_call(
        qkv_kernel,
        in_specs=[SMEM] + [ANY] * 12,
        out_specs=[ANY] * 9,
        out_shape=qkv_shapes(REQ) + qkv_shapes(REQ) + [
            jax.ShapeDtypeStruct((REQ, ROWS, WIDTH), jnp.bfloat16),
            jax.ShapeDtypeStruct((WO_EARLY, WIDTH), jnp.bfloat16),
            jax.ShapeDtypeStruct((384 - WO_EARLY, WIDTH), jnp.bfloat16),
        ],
        scratch_shapes=[
            pltpu.VMEM((2, REQ, ROWS, WIDTH), jnp.bfloat16),
            pltpu.VMEM((2, REQ, ROWS, WIDTH), jnp.bfloat16),
            pltpu.VMEM((384 - WO_EARLY, WIDTH), jnp.bfloat16),
            *SHARED_SCRATCH, *qkv_scratch(REQ), *qkv_scratch(REQ),
            DMA, DMA((REQ,)), DMA((REQ,)), DMA((REQ,)), DMA((REQ,)), DMA((REQ,)), DMA((REQ,)), DMA((REQ,)), DMA, DMA, DMA((2,)),
        ],
        compiler_params=pltpu.CompilerParams(collective_id=0, has_side_effects=True),
        cost_estimate=pl.CostEstimate(flops=2 * 10 ** 9, bytes_accessed=60 * 10 ** 6, transcendentals=0),
        name="project_rows",
    )(prefix, x_rows, *shared, w_o)


BLOCK_KV = 512
WINDOW = 272


def attn_kernel(prefix_ref, valid_ref, qa_ref, ka_ref, va_ref, qb_ref, kb_ref, vb_ref, k_ref, v_ref, *refs):
    o_ref, ko_ref, vo_ref, kbuf, vbuf, obuf, qa, ka, va, qb, kb, vb, qbuf, fbuf, acc_ref, m_ref, l_ref, even_ref, odd_ref, k_sem, v_sem, out_sem, in_sem = refs
    n_req, heads = REQ, 3
    rows, dim = 4 * ROWS, HEAD
    slots = kbuf.shape[1]
    chip = lax.axis_index("tp") // 2
    ours = pl.ds(pl.multiple_of(chip * 2 * ROWS, 2 * ROWS), 2 * ROWS)
    theirs = pl.ds(pl.multiple_of((1 - chip) * 2 * ROWS, 2 * ROWS), 2 * ROWS)
    last = slots // BLOCK_KV - 1
    factor = (dim ** -0.5) * LOG2E

    def copies(r):
        return (
            (pltpu.make_async_copy(k_ref.at[r], kbuf.at[r], k_sem.at[r]), pltpu.make_async_copy(v_ref.at[r], vbuf.at[r], v_sem.at[r])),
            (pltpu.make_async_copy(kbuf.at[r], ko_ref.at[r], out_sem.at[0, r]), pltpu.make_async_copy(vbuf.at[r], vo_ref.at[r], out_sem.at[1, r])),
            pltpu.make_async_copy(obuf.at[r], o_ref.at[r], out_sem.at[2, r]),
        )

    news = (
        pltpu.make_async_copy(ka_ref, ka, in_sem.at[0]),
        pltpu.make_async_copy(kb_ref, kb, in_sem.at[1]),
        pltpu.make_async_copy(va_ref, va, in_sem.at[2]),
        pltpu.make_async_copy(vb_ref, vb, in_sem.at[3]),
        pltpu.make_async_copy(qa_ref, qa, in_sem.at[4]),
        pltpu.make_async_copy(qb_ref, qb, in_sem.at[5]),
    )

    def merge(mine, far, buf, r, start, count):
        base = pl.multiple_of(jnp.minimum((start // 16) * 16, slots - WINDOW), 16)
        shift = start - base
        fbuf[ours, :] = mine.astype(jnp.float32)
        fbuf[theirs, :] = far.astype(jnp.float32)
        rolled = pltpu.roll(fbuf[...], shift, 0)
        idx = lax.broadcasted_iota(jnp.int32, rolled.shape, 0) - shift
        window = buf[r, pl.ds(base, WINDOW), :].astype(jnp.float32)
        merged = jnp.where((idx >= 0) & (idx < count), rolled, window)
        buf[r, pl.ds(base, WINDOW), :] = merged.astype(jnp.bfloat16)

    for copy in news:
        copy.start()
    for r in range(2):
        for load in copies(r)[0]:
            load.start()
    fbuf[rows:, :] = jnp.zeros((WINDOW - rows, dim), jnp.float32)
    for copy in news:
        copy.wait()

    @pl.loop(0, n_req)
    def _(r):
        start = prefix_ref[r]
        count = valid_ref[r]
        loads, stores, give = copies(r)
        for load in loads:
            load.wait()

        @pl.when(r + 2 < n_req)
        def _():
            for load in copies(r + 2)[0]:
                load.start()

        merge(ka[r], kb[r], kbuf, r, start, count)
        merge(va[r], vb[r], vbuf, r, start, count)
        for store in stores:
            store.start()
        acc_ref[...] = jnp.zeros_like(acc_ref)
        l_ref[...] = jnp.zeros_like(l_ref)
        m_ref[...] = jnp.full_like(m_ref, -1.0e30)
        n_full = start // BLOCK_KV
        n_all = (start + count + BLOCK_KV - 1) // BLOCK_KV
        for h in range(heads):
            qbuf[h, ours, :] = qa[r, h]
            qbuf[h, theirs, :] = qb[r, h]
        wide = qbuf[...].reshape(heads * rows, dim).astype(jnp.float32) * factor
        high = wide.astype(jnp.bfloat16)
        low = (wide - high.astype(jnp.float32)).astype(jnp.bfloat16)
        queries = jnp.concatenate([high, low], axis=1)

        def scores(blk, dst):
            off = pl.multiple_of(jnp.minimum(blk, last) * BLOCK_KV, BLOCK_KV)
            keys = kbuf[r, pl.ds(off, BLOCK_KV), :]
            keys = jnp.concatenate([keys, keys], axis=1)
            s = lax.dot_general(queries, keys, (((1,), (1,)), ((), ())), preferred_element_type=jnp.float32)
            dst[...] = s

        def absorb(blk, src, masked):
            off = pl.multiple_of(blk * BLOCK_KV, BLOCK_KV)
            vals = vbuf[r, pl.ds(off, BLOCK_KV), :]
            s = src[...]
            if masked:
                row = lax.broadcasted_iota(jnp.int32, (rows, BLOCK_KV), 0)
                col = lax.broadcasted_iota(jnp.int32, (rows, BLOCK_KV), 1)
                visible = col + off <= start + jnp.minimum(row, count - 1)
                s = jnp.where(jnp.concatenate([visible] * heads, axis=0), s, -1.0e30)
            m_old = m_ref[...]
            best = jnp.max(s, axis=1, keepdims=True)
            m_new = jnp.maximum(m_old, best)
            alpha = jnp.exp2(m_old - m_new)
            p = jnp.exp2(s - m_new[:, :1])
            part = p[:, :128]
            for j in range(1, BLOCK_KV // 128):
                part = part + p[:, j * 128:(j + 1) * 128]
            l_ref[...] = l_ref[...] * alpha + part
            m_ref[...] = m_new
            acc_ref[...] = acc_ref[...] * alpha + jnp.dot(p.astype(jnp.bfloat16), vals, preferred_element_type=jnp.float32)

        def step(blk, masked):
            @pl.when(blk % 2 == 0)
            def _():
                scores(blk + 1, odd_ref)
                absorb(blk, even_ref, masked)

            @pl.when(blk % 2 == 1)
            def _():
                scores(blk + 1, even_ref)
                absorb(blk, odd_ref, masked)

        scores(0, even_ref)

        @pl.loop(0, n_full)
        def _(blk):
            step(blk, False)

        @pl.loop(n_full, n_all)
        def _(blk):
            step(blk, True)

        for h in range(heads):
            at = slice(h * rows, (h + 1) * rows)
            total = jnp.sum(l_ref[at], axis=1, keepdims=True)
            obuf[r, :, h * dim:(h + 1) * dim] = (acc_ref[at] / total).astype(jnp.bfloat16)
        give.start()

    @pl.loop(0, n_req)
    def _(r):
        _, stores, give = copies(r)
        for store in stores:
            store.wait()
        give.wait()


def attention(prefix, valid, mine, far, k_cache, v_cache):
    part = (REQ, 2 * ROWS, HEAD)
    state = pltpu.VMEM((3 * 4 * ROWS, HEAD), jnp.float32)
    tile = pltpu.VMEM((3 * 4 * ROWS, BLOCK_KV), jnp.float32)
    slots = pltpu.VMEM((REQ,) + k_cache.shape[1:], jnp.bfloat16)
    q_part = pltpu.VMEM((REQ, 3, 2 * ROWS, HEAD), jnp.bfloat16)
    kv_part = pltpu.VMEM(part, jnp.bfloat16)
    return pl.pallas_call(
        attn_kernel,
        in_specs=[SMEM, SMEM] + [ANY] * 8,
        out_specs=[ANY, ANY, ANY],
        scratch_shapes=[
            slots, slots, pltpu.VMEM((REQ, 4 * ROWS, 3 * HEAD), jnp.bfloat16),
            q_part, kv_part, kv_part, q_part, kv_part, kv_part,
            pltpu.VMEM((3, 4 * ROWS, HEAD), jnp.bfloat16),
            pltpu.VMEM((WINDOW, HEAD), jnp.float32),
            state, state, state, tile, tile,
            DMA((REQ,)), DMA((REQ,)), DMA((3, REQ)), DMA((6,)),
        ],
        out_shape=[
            jax.ShapeDtypeStruct((REQ, 4 * ROWS, 3 * HEAD), jnp.bfloat16),
            jax.ShapeDtypeStruct(k_cache.shape, jnp.bfloat16),
            jax.ShapeDtypeStruct(v_cache.shape, jnp.bfloat16),
        ],
        cost_estimate=pl.CostEstimate(flops=10 ** 10, bytes_accessed=40 * 10 ** 6, transcendentals=7 * 10 ** 6),
        compiler_params=pltpu.CompilerParams(vmem_limit_bytes=67_043_328),
        name="attention",
    )(prefix, valid, *mine, *far, k_cache, v_cache)


def mlp_kernel(o_ref, x_ref, pair_ref, g_ref, wo_ref, early_ref, far_ref, wg_ref, wu_ref, wd_ref, out_ref,
               osrc, obuf, xin, wo, wg, wu, wd, hbuf, ubuf, psend, precv, pown, xsend, xrecv, x1buf, outbuf,
               w_sem, wl_sem, in_sem, o_sem, so, ro, lo, swc, rwc, sh, rh, sp, rp, ss, rs):
    dp, peers = partners()
    me, core_peer, chip_peer, far_peer = peers

    def cols(who):
        return pl.ds(pl.multiple_of(who * 384, 384), 384)

    def share(k, s):
        slot, first, n = STEPS[k]
        block = peers[s] if slot == 0 else peers[s ^ 2]
        src = (o_ref if s == 0 else osrc).at[pl.ds(first, n), block]
        dst = obuf.at[slot, pl.ds(first, n), :, cols(me)]
        if s == 0:
            return pltpu.make_async_copy(src, dst, lo.at[k])
        return send(src, dst, so.at[k, s - 1], ro.at[k, s - 1], (dp, peers[s]))

    def wo_rows(who, first, count):
        return wo.at[pl.ds(pl.multiple_of(who * 384 + first, 32), count)]

    have = (
        (wo_ref, wo_rows(me, 0, 384)),
        (early_ref, wo_rows(chip_peer, 0, WO_EARLY)),
        (far_ref, wo_rows(chip_peer, WO_EARLY, 384 - WO_EARLY)),
    )
    wo_local = tuple(pltpu.make_async_copy(src, dst, wl_sem.at[i]) for i, (src, dst) in enumerate(have))
    wo_core = tuple(send(src, dst, swc.at[i], rwc.at[i], (dp, core_peer)) for i, (src, dst) in enumerate(have))
    weights = (
        pltpu.make_async_copy(wg_ref, wg.at[pl.ds(0, FFN)], w_sem.at[0]),
        pltpu.make_async_copy(wu_ref, wu.at[pl.ds(0, FFN)], w_sem.at[1]),
        pltpu.make_async_copy(wd_ref, wd.at[pl.ds(0, FFN)], w_sem.at[2]),
    )
    x_loads = (
        pltpu.make_async_copy(x_ref, xin.at[0], in_sem.at[0]),
        pltpu.make_async_copy(pair_ref, xin.at[1], in_sem.at[1]),
    )
    steps = range(len(STEPS))

    load_o = pltpu.make_async_copy(o_ref, osrc, in_sem.at[2])
    load_o.start()
    for copy in wo_local + x_loads:
        copy.start()
    greet([(dp, core_peer), (dp, chip_peer), (dp, far_peer)])
    load_o.wait()
    for k in steps:
        for s in (2, 3, 1):
            share(k, s).start()
    for copy in wo_core:
        copy.start()
    for k in steps:
        share(k, 0).start()
    pad = jnp.zeros((FFN_PAD - FFN, WIDTH), jnp.bfloat16)
    for buf in (wg, wu, wd):
        buf[FFN:, :] = pad

    gain = g_ref[...].astype(jnp.float32).reshape(1, WIDTH)

    def half_rows(k):
        return STEPS[k][2] * ROWS

    def give_h(k):
        mine = hbuf.at[pl.ds(2 * STEP_ROWS[k], half_rows(k))]
        theirs = hbuf.at[pl.ds(2 * STEP_ROWS[k] + half_rows(k), half_rows(k))]
        return send(mine, theirs, sh.at[k], rh.at[k], (dp, core_peer))

    def part(n):
        return pl.ds(pl.multiple_of(n * HALF_WIDTH, HALF_WIDTH), HALF_WIDTH)

    def give_p(k, n):
        at = pl.ds(STEP_ROWS[k], half_rows(k))
        return send(psend.at[at, part(n)], precv.at[at, part(n)], sp.at[k, n], rp.at[k, n], (dp, core_peer))

    def give_s(k, n):
        at = pl.ds(STEPS[k][1] * ROWS, half_rows(k))
        return send(xsend.at[at, part(n)], xrecv.at[at, part(n)], ss.at[k, n], rs.at[k, n], (dp, chip_peer))

    def give_out(k, n):
        reqs = pl.ds(STEPS[k][1], STEPS[k][2])
        return pltpu.make_async_copy(outbuf.at[reqs, :, part(n)], out_ref.at[reqs, :, part(n)], o_sem.at[k, n])

    def attn_out(k):
        slot, first, n = STEPS[k]
        m = half_rows(k)
        for s in (2, 3, 1):
            share(k, s).wait_recv()
        share(k, 0).wait()
        heads = obuf[slot, first:first + n].reshape(m, WIDTH)
        attn = jnp.dot(heads, wo[...], preferred_element_type=jnp.float32).astype(jnp.bfloat16)
        base = xin[slot, first:first + n].reshape(m, WIDTH)
        mid = (base.astype(jnp.float32) + attn.astype(jnp.float32)).astype(jnp.bfloat16)
        if slot == 0:
            x1buf[first * ROWS:first * ROWS + m] = mid
        hbuf[2 * STEP_ROWS[k]:2 * STEP_ROWS[k] + m] = rms_norm(mid.astype(jnp.float32), gain)
        give_h(k).start()

    def widen(k):
        give_h(k).wait_recv()
        if k == 0:
            weights[0].wait()
            weights[1].wait()
        rows = pl.ds(2 * STEP_ROWS[k], 2 * half_rows(k))

        @pl.loop(0, FFN_PAD // FFN_TILE)
        def _(f):
            at = pl.ds(pl.multiple_of(f * FFN_TILE, FFN_TILE), FFN_TILE)
            nt = (((1,), (1,)), ((), ()))
            gate = lax.dot_general(hbuf[rows, :], wg[at, :], nt, preferred_element_type=jnp.float32)
            up = lax.dot_general(hbuf[rows, :], wu[at, :], nt, preferred_element_type=jnp.float32)
            ubuf[:2 * half_rows(k), at] = (jax.nn.silu(gate) * up).astype(jnp.bfloat16)

    def narrow(k):
        m = half_rows(k)
        at = slice(STEP_ROWS[k], STEP_ROWS[k] + m)
        if k == 0:
            weights[2].wait()

        @pl.loop(0, 2)
        def _(n):
            down = jnp.dot(ubuf[:2 * m, :], wd[:, part(n)], preferred_element_type=jnp.float32)
            pown[at, part(n)] = down[:m]
            psend[at, part(n)] = down[m:].astype(jnp.bfloat16)
            give_p(k, n).start()

    def combine(k):
        slot, first, count = STEPS[k]
        m = half_rows(k)
        at = slice(STEP_ROWS[k], STEP_ROWS[k] + m)
        mine = slice(first * ROWS, first * ROWS + m)

        @pl.loop(0, 2)
        def _(n):
            give_p(k, n).wait_recv()
            total = pown[at, part(n)] + precv[at, part(n)].astype(jnp.float32)
            if slot == 1:
                xsend[mine, part(n)] = total.astype(jnp.bfloat16)
                give_s(k, n).start()
            else:
                for j in RS_NEED[k]:
                    give_s(j, n).wait_recv()
                down = (total + xrecv[mine, part(n)].astype(jnp.float32)).astype(jnp.bfloat16)
                out = (x1buf[mine, part(n)].astype(jnp.float32) + down.astype(jnp.float32)).astype(jnp.bfloat16)
                outbuf[first:first + count, :, part(n)] = out.reshape(count, ROWS, HALF_WIDTH)
                give_out(k, n).start()

    for copy in wo_local + x_loads:
        copy.wait()
    for copy in weights:
        copy.start()
    for copy in wo_core:
        copy.wait_recv()
    attn_out(0)
    for k in steps:
        widen(k)
        if k + 1 < len(STEPS):
            attn_out(k + 1)
        if k > 0:
            combine(k - 1)
        narrow(k)
    combine(len(STEPS) - 1)
    for copy in wo_core:
        copy.wait_send()
    for k in steps:
        for s in (2, 3, 1):
            share(k, s).wait_send()
        give_h(k).wait_send()
        for n in range(2):
            give_p(k, n).wait_send()
            if STEPS[k][0] == 1:
                give_s(k, n).wait_send()
            else:
                give_out(k, n).wait()


def finish_layer(*operands):
    return pl.pallas_call(
        mlp_kernel,
        in_specs=[ANY] * 3 + [VMEM] + [ANY] * 6,
        out_specs=ANY,
        out_shape=jax.ShapeDtypeStruct((REQ, ROWS, WIDTH), jnp.bfloat16),
        scratch_shapes=[
            pltpu.VMEM((REQ, 4, ROWS, 3 * HEAD), jnp.bfloat16),
            pltpu.VMEM((2, REQ, ROWS, WIDTH), jnp.bfloat16),
            pltpu.VMEM((2, REQ, ROWS, WIDTH), jnp.bfloat16),
            pltpu.VMEM((WIDTH, WIDTH), jnp.bfloat16),
            pltpu.VMEM((FFN_PAD, WIDTH), jnp.bfloat16),
            pltpu.VMEM((FFN_PAD, WIDTH), jnp.bfloat16),
            pltpu.VMEM((FFN_PAD, WIDTH), jnp.bfloat16),
            pltpu.VMEM((2 * ALL_ROWS, WIDTH), jnp.bfloat16),
            pltpu.VMEM((MAX_ROWS, FFN_PAD), jnp.bfloat16),
            pltpu.VMEM((ALL_ROWS, WIDTH), jnp.bfloat16),
            pltpu.VMEM((ALL_ROWS, WIDTH), jnp.bfloat16),
            pltpu.VMEM((ALL_ROWS, WIDTH), jnp.float32),
            pltpu.VMEM((REQ * ROWS, WIDTH), jnp.bfloat16),
            pltpu.VMEM((REQ * ROWS, WIDTH), jnp.bfloat16),
            pltpu.VMEM((REQ * ROWS, WIDTH), jnp.bfloat16),
            pltpu.VMEM((REQ, ROWS, WIDTH), jnp.bfloat16),
            DMA((3,)), DMA((3,)), DMA((3,)), DMA((5, 2)),
            DMA((5, 3)), DMA((5, 3)), DMA((5,)),
            DMA((3,)), DMA((3,)),
            DMA((5,)), DMA((5,)), DMA((5, 2)), DMA((5, 2)), DMA((3, 2)), DMA((3, 2)),
        ],
        compiler_params=pltpu.CompilerParams(collective_id=1, has_side_effects=True, vmem_limit_bytes=62 * 1024 * 1024),
        name="finish_layer",
    )(*operands)


def solution(mesh):
    row_spec = P("dp", "tp", None)
    cache_spec = P("dp", None, "tp", None)
    req_spec = P("dp")
    rep_spec = P(None)
    col_spec = P(None, "tp")
    bias_spec = P("tp")
    down_spec = P("tp", None)

    def layer(x_rows, k_cache, v_cache, prefix, valid, g_attn, w_q, b_q, w_k, b_k, w_v, b_v, w_o, g_mlp, w_gate, w_up, w_down):
        cache_shape = (REQ, k_cache.shape[1], HEAD)
        k_old, v_old = k_cache.reshape(cache_shape), v_cache.reshape(cache_shape)
        across_chips = [(0, 2), (1, 3), (2, 0), (3, 1)]
        shared = (g_attn, b_q, b_k, b_v) + rope_tables() + (w_q, w_k, w_v)
        *qkv, x_pair, w_early, w_late = project_rows(prefix, x_rows, shared, w_o)
        mine, far = qkv[:3], qkv[3:]
        w_own, far[0] = lax.optimization_barrier((w_late, far[0]))
        w_far = lax.ppermute(w_own, "tp", across_chips)
        o, k_out, v_out = attention(prefix, valid, mine, far, k_old, v_old)
        x_out = finish_layer(o.reshape(REQ, 4, ROWS, 3 * HEAD), x_rows, x_pair, g_mlp, w_o, w_early, w_far, w_gate.T, w_up.T, w_down)
        return x_out, k_out.reshape(k_cache.shape), v_out.reshape(v_cache.shape)

    in_specs = (row_spec, cache_spec, cache_spec, req_spec, req_spec, rep_spec, col_spec, bias_spec, col_spec, bias_spec, col_spec, bias_spec, down_spec, rep_spec, col_spec, col_spec, down_spec)
    return jax.shard_map(layer, mesh=mesh, in_specs=in_specs, out_specs=(row_spec, cache_spec, cache_spec), check_vma=False)
```

```python
import jax
import jax.numpy as jnp
import numpy as np
from jax import lax
from jax.experimental import pallas as pl
from jax.experimental.pallas import tpu as pltpu
from jax.sharding import PartitionSpec as P

ROPE_THETA = 1.0e6
NORM_EPS = 1.0e-6
LOG2E = 1.4426950408889634
MESH = pl.DeviceIdType.MESH
ANY = pl.BlockSpec(memory_space=pl.ANY)
VMEM = pl.BlockSpec(memory_space=pltpu.VMEM)
SMEM = pl.BlockSpec(memory_space=pltpu.SMEM)
DMA = pltpu.SemaphoreType.DMA
REQ = 6
ROWS = 64
WIDTH = 1536
HEAD = 128
FFN = 2240
FFN_PAD = 2304
FFN_TILE = 768
WO_EARLY = 32
STEPS = ((1, 0, 2), (1, 2, 2), (1, 4, 2), (0, 0, 3), (0, 3, 3))
STEP_ROWS = [ROWS * sum(n for _, _, n in STEPS[:k]) for k in range(len(STEPS))]
RS_NEED = {3: (0, 1), 4: (2,)}
ALL_ROWS = 2 * REQ * ROWS
MAX_ROWS = 2 * ROWS * max(n for _, _, n in STEPS)
HALF_WIDTH = 768


def rms_norm(wide, gain):
    inv_rms = lax.rsqrt(jnp.mean(wide * wide, axis=-1, keepdims=True) + NORM_EPS)
    return (wide * inv_rms * gain).astype(jnp.bfloat16)


def partners():
    me = lax.axis_index("tp")
    chip, core = me // 2, me % 2
    return lax.axis_index("dp"), (me, chip * 2 + 1 - core, (1 - chip) * 2 + core, (1 - chip) * 2 + 1 - core)


def greet(devices):
    barrier = pltpu.get_barrier_semaphore()
    for device in devices:
        pl.semaphore_signal(barrier, inc=1, device_id=device, device_id_type=MESH)
    pl.semaphore_wait(barrier, len(devices))


def send(src, dst, send_sem, recv_sem, device):
    return pltpu.make_async_remote_copy(src_ref=src, dst_ref=dst, send_sem=send_sem, recv_sem=recv_sem, device_id=device, device_id_type=MESH)


def rope_tables():
    freq = ROPE_THETA ** (-(np.arange(HEAD // 2, dtype=np.float64) * 2.0) / HEAD)
    freq = np.concatenate([freq, freq])
    angles = np.arange(4 * ROWS, dtype=np.float64)[:, None] * freq
    return np.cos(angles).astype(np.float32), np.sin(angles).astype(np.float32), freq.astype(np.float32)[None]


def load_shared(refs, bufs, sem):
    gain, bq, bk, bv, cos, sin, freq, wq, wk, wv = refs
    small, wbuf = bufs[:7], bufs[7]
    pairs = list(zip((gain, bq, bk, bv, cos, sin, freq), small))
    pairs += [(wq, wbuf.at[:, pl.ds(0, 384)]), (wk, wbuf.at[:, pl.ds(384, 128)]), (wv, wbuf.at[:, pl.ds(512, 128)])]
    return [pltpu.make_async_copy(src, dst, sem.at[i]) for i, (src, dst) in enumerate(pairs)]


SHARED_SCRATCH = [
    pltpu.VMEM((WIDTH,), jnp.bfloat16), pltpu.VMEM((384,), jnp.bfloat16), pltpu.VMEM((128,), jnp.bfloat16), pltpu.VMEM((128,), jnp.bfloat16),
    pltpu.VMEM((4 * ROWS, HEAD), jnp.float32), pltpu.VMEM((4 * ROWS, HEAD), jnp.float32), pltpu.VMEM((1, HEAD), jnp.float32),
    pltpu.VMEM((WIDTH, 640), jnp.bfloat16), DMA((10,)),
]


def qkv_scratch(n_req):
    return [
        pltpu.VMEM((n_req, 3, 2 * ROWS, HEAD), jnp.bfloat16),
        pltpu.VMEM((n_req, 2 * ROWS, HEAD), jnp.bfloat16),
        pltpu.VMEM((n_req, 2 * ROWS, HEAD), jnp.bfloat16),
        DMA((3, n_req)),
    ]


def give_qkv(bufs, refs, sem, r):
    return [pltpu.make_async_copy(buf.at[r], ref.at[r], sem.at[i, r]) for i, (buf, ref) in enumerate(zip(bufs, refs))]


def project(x, position, chip, shared, outs, r):
    g_ref, *biases, cos_ref, sin_ref, freq_ref, wbuf = shared
    q_ref, k_ref, v_ref = outs
    rows = pl.ds(pl.multiple_of(chip * 2 * ROWS, 2 * ROWS), 2 * ROWS)
    normed = rms_norm(x.astype(jnp.float32), g_ref[...].astype(jnp.float32).reshape(1, WIDTH))
    total = jnp.dot(normed, wbuf[...], preferred_element_type=jnp.float32)
    angle = jnp.full((8, HEAD), position, jnp.int32).astype(jnp.float32) * freq_ref[...]
    cos_p, sin_p = jnp.cos(angle)[:1], jnp.sin(angle)[:1]
    cos_i, sin_i = cos_ref[rows, :], sin_ref[rows, :]
    cos_t = cos_p * cos_i - sin_p * sin_i
    sin_t = sin_p * cos_i + cos_p * sin_i
    lane = lax.broadcasted_iota(jnp.int32, sin_t.shape, 1)
    sin_t = jnp.where(lane < HEAD // 2, -sin_t, sin_t)
    bias = jnp.concatenate([b[...].astype(jnp.float32).reshape(1, b.shape[0]) for b in biases], axis=1)
    rounded = (total + bias).astype(jnp.bfloat16)
    for head in range(4):
        part = rounded[:, head * HEAD:(head + 1) * HEAD].astype(jnp.float32)
        turned = (part * cos_t + pltpu.roll(part, HEAD // 2, 1) * sin_t).astype(jnp.bfloat16)
        if head < 3:
            q_ref[r, head] = turned
        else:
            k_ref[r] = turned
    v_ref[r] = rounded[:, 4 * HEAD:]


def qkv_kernel(prefix_ref, x_ref, *refs):
    shared_refs, wo_ref, mine_refs, far_refs, pair_ref, early_ref = refs[:10], refs[10], refs[11:14], refs[14:17], refs[17], refs[18]
    late_ref, own, other, late = refs[19:23]
    shared, shared_sem = refs[23:31], refs[31]
    mine, mine_sem = refs[32:35], refs[35]
    far, far_sem = refs[36:39], refs[39]
    in_sem, out_sem, sx, rx, sc, rc, sf, rf, se, re, late_sem = refs[40:]
    dp, (me, core_peer, chip_peer, _) = partners()
    chip, core = me // 2, me % 2
    load_x = pltpu.make_async_copy(x_ref, own.at[core], in_sem)
    load_x.start()
    loads = load_shared(shared_refs, shared, shared_sem)
    greet([(dp, core_peer), (dp, chip_peer)])
    load_x.wait()

    def to_chip(r):
        return send(own.at[core, r], other.at[core, r], sx.at[r], rx.at[r], (dp, chip_peer))

    def to_core(r):
        return send(own.at[core, r], own.at[core, r], sc.at[r], rc.at[r], (dp, core_peer))

    def forward(r):
        return send(other.at[core, r], other.at[core, r], sf.at[r], rf.at[r], (dp, core_peer))

    def keep(r):
        return pltpu.make_async_copy(other.at[core, r], pair_ref.at[r], out_sem.at[r])

    early = send(wo_ref.at[pl.ds(0, WO_EARLY)], early_ref, se, re, (dp, chip_peer))
    for r in range(REQ):
        to_chip(r).start()
    early.start()
    for r in range(REQ):
        to_core(r).start()
    take_late = pltpu.make_async_copy(wo_ref.at[pl.ds(WO_EARLY, 384 - WO_EARLY)], late, late_sem.at[0])
    give_late = pltpu.make_async_copy(late, late_ref, late_sem.at[1])
    for load in loads:
        load.start()
    take_late.start()
    for load in loads:
        load.wait()
    take_late.wait()
    give_late.start()

    @pl.loop(0, REQ)
    def _(r):
        to_core(r).wait_recv()
        project(own[:, r].reshape(2 * ROWS, WIDTH), prefix_ref[r], chip, shared, mine, r)
        for copy in give_qkv(mine, mine_refs, mine_sem, r):
            copy.start()

    @pl.loop(0, REQ + 1)
    def _(r):
        @pl.when(r < REQ)
        def _():
            to_chip(r).wait_recv()
            forward(r).start()
            keep(r).start()

        @pl.when(r > 0)
        def _():
            forward(r - 1).wait_recv()
            project(other[:, r - 1].reshape(2 * ROWS, WIDTH), prefix_ref[r - 1], 1 - chip, shared, far, r - 1)
            for copy in give_qkv(far, far_refs, far_sem, r - 1):
                copy.start()

    early.wait()
    give_late.wait()

    @pl.loop(0, REQ)
    def _(r):
        to_core(r).wait_send()
        for copy in give_qkv(mine, mine_refs, mine_sem, r):
            copy.wait()
        to_chip(r).wait_send()
        forward(r).wait_send()
        keep(r).wait()
        for copy in give_qkv(far, far_refs, far_sem, r):
            copy.wait()


def qkv_shapes(n_req):
    return [
        jax.ShapeDtypeStruct((n_req, 3, 2 * ROWS, HEAD), jnp.bfloat16),
        jax.ShapeDtypeStruct((n_req, 2 * ROWS, HEAD), jnp.bfloat16),
        jax.ShapeDtypeStruct((n_req, 2 * ROWS, HEAD), jnp.bfloat16),
    ]


def project_rows(prefix, x_rows, shared, w_o):
    return pl.pallas_call(
        qkv_kernel,
        in_specs=[SMEM] + [ANY] * 12,
        out_specs=[ANY] * 9,
        out_shape=qkv_shapes(REQ) + qkv_shapes(REQ) + [
            jax.ShapeDtypeStruct((REQ, ROWS, WIDTH), jnp.bfloat16),
            jax.ShapeDtypeStruct((WO_EARLY, WIDTH), jnp.bfloat16),
            jax.ShapeDtypeStruct((384 - WO_EARLY, WIDTH), jnp.bfloat16),
        ],
        scratch_shapes=[
            pltpu.VMEM((2, REQ, ROWS, WIDTH), jnp.bfloat16),
            pltpu.VMEM((2, REQ, ROWS, WIDTH), jnp.bfloat16),
            pltpu.VMEM((384 - WO_EARLY, WIDTH), jnp.bfloat16),
            *SHARED_SCRATCH, *qkv_scratch(REQ), *qkv_scratch(REQ),
            DMA, DMA((REQ,)), DMA((REQ,)), DMA((REQ,)), DMA((REQ,)), DMA((REQ,)), DMA((REQ,)), DMA((REQ,)), DMA, DMA, DMA((2,)),
        ],
        compiler_params=pltpu.CompilerParams(collective_id=0, has_side_effects=True),
        cost_estimate=pl.CostEstimate(flops=2 * 10 ** 9, bytes_accessed=60 * 10 ** 6, transcendentals=0),
        name="project_rows",
    )(prefix, x_rows, *shared, w_o)


BLOCK_KV = 512
WINDOW = 272


def attn_kernel(prefix_ref, valid_ref, qa_ref, ka_ref, va_ref, qb_ref, kb_ref, vb_ref, k_ref, v_ref, *refs):
    o_ref, ko_ref, vo_ref, kbuf, vbuf, obuf, qa, ka, va, qb, kb, vb, qbuf, fbuf, acc_ref, m_ref, l_ref, even_ref, odd_ref, k_sem, v_sem, out_sem, in_sem = refs
    n_req, heads = REQ, 3
    rows, dim = 4 * ROWS, HEAD
    slots = kbuf.shape[1]
    chip = lax.axis_index("tp") // 2
    ours = pl.ds(pl.multiple_of(chip * 2 * ROWS, 2 * ROWS), 2 * ROWS)
    theirs = pl.ds(pl.multiple_of((1 - chip) * 2 * ROWS, 2 * ROWS), 2 * ROWS)
    last = slots // BLOCK_KV - 1
    factor = (dim ** -0.5) * LOG2E

    def copies(r):
        return (
            (pltpu.make_async_copy(k_ref.at[r], kbuf.at[r], k_sem.at[r]), pltpu.make_async_copy(v_ref.at[r], vbuf.at[r], v_sem.at[r])),
            (pltpu.make_async_copy(kbuf.at[r], ko_ref.at[r], out_sem.at[0, r]), pltpu.make_async_copy(vbuf.at[r], vo_ref.at[r], out_sem.at[1, r])),
            pltpu.make_async_copy(obuf.at[r], o_ref.at[r], out_sem.at[2, r]),
        )

    news = (
        pltpu.make_async_copy(ka_ref, ka, in_sem.at[0]),
        pltpu.make_async_copy(kb_ref, kb, in_sem.at[1]),
        pltpu.make_async_copy(va_ref, va, in_sem.at[2]),
        pltpu.make_async_copy(vb_ref, vb, in_sem.at[3]),
        pltpu.make_async_copy(qa_ref, qa, in_sem.at[4]),
        pltpu.make_async_copy(qb_ref, qb, in_sem.at[5]),
    )

    def merge(mine, far, buf, r, start, count):
        base = pl.multiple_of(jnp.minimum((start // 16) * 16, slots - WINDOW), 16)
        shift = start - base
        fbuf[ours, :] = mine.astype(jnp.float32)
        fbuf[theirs, :] = far.astype(jnp.float32)
        rolled = pltpu.roll(fbuf[...], shift, 0)
        idx = lax.broadcasted_iota(jnp.int32, rolled.shape, 0) - shift
        window = buf[r, pl.ds(base, WINDOW), :].astype(jnp.float32)
        merged = jnp.where((idx >= 0) & (idx < count), rolled, window)
        buf[r, pl.ds(base, WINDOW), :] = merged.astype(jnp.bfloat16)

    for copy in news:
        copy.start()
    for r in range(2):
        for load in copies(r)[0]:
            load.start()
    fbuf[rows:, :] = jnp.zeros((WINDOW - rows, dim), jnp.float32)
    for copy in news:
        copy.wait()

    @pl.loop(0, n_req)
    def _(r):
        start = prefix_ref[r]
        count = valid_ref[r]
        loads, stores, give = copies(r)
        for load in loads:
            load.wait()

        @pl.when(r + 2 < n_req)
        def _():
            for load in copies(r + 2)[0]:
                load.start()

        merge(ka[r], kb[r], kbuf, r, start, count)
        merge(va[r], vb[r], vbuf, r, start, count)
        for store in stores:
            store.start()
        acc_ref[...] = jnp.zeros_like(acc_ref)
        l_ref[...] = jnp.zeros_like(l_ref)
        m_ref[...] = jnp.full_like(m_ref, -1.0e30)
        n_full = start // BLOCK_KV
        n_all = (start + count + BLOCK_KV - 1) // BLOCK_KV
        for h in range(heads):
            qbuf[h, ours, :] = qa[r, h]
            qbuf[h, theirs, :] = qb[r, h]
        wide = qbuf[...].reshape(heads * rows, dim).astype(jnp.float32) * factor
        high = wide.astype(jnp.bfloat16)
        low = (wide - high.astype(jnp.float32)).astype(jnp.bfloat16)
        queries = jnp.concatenate([high, low], axis=1)

        def scores(blk, dst):
            off = pl.multiple_of(jnp.minimum(blk, last) * BLOCK_KV, BLOCK_KV)
            keys = kbuf[r, pl.ds(off, BLOCK_KV), :]
            keys = jnp.concatenate([keys, keys], axis=1)
            s = lax.dot_general(queries, keys, (((1,), (1,)), ((), ())), preferred_element_type=jnp.float32)
            dst[...] = s

        def absorb(blk, src, masked):
            off = pl.multiple_of(blk * BLOCK_KV, BLOCK_KV)
            vals = vbuf[r, pl.ds(off, BLOCK_KV), :]
            s = src[...]
            if masked:
                row = lax.broadcasted_iota(jnp.int32, (rows, BLOCK_KV), 0)
                col = lax.broadcasted_iota(jnp.int32, (rows, BLOCK_KV), 1)
                visible = col + off <= start + jnp.minimum(row, count - 1)
                s = jnp.where(jnp.concatenate([visible] * heads, axis=0), s, -1.0e30)
            m_old = m_ref[...]
            best = jnp.max(s, axis=1, keepdims=True)
            m_new = jnp.maximum(m_old, best)
            alpha = jnp.exp2(m_old - m_new)
            p = jnp.exp2(s - m_new[:, :1])
            part = p[:, :128]
            for j in range(1, BLOCK_KV // 128):
                part = part + p[:, j * 128:(j + 1) * 128]
            l_ref[...] = l_ref[...] * alpha + part
            m_ref[...] = m_new
            acc_ref[...] = acc_ref[...] * alpha + jnp.dot(p.astype(jnp.bfloat16), vals, preferred_element_type=jnp.float32)

        def step(blk, masked):
            @pl.when(blk % 2 == 0)
            def _():
                scores(blk + 1, odd_ref)
                absorb(blk, even_ref, masked)

            @pl.when(blk % 2 == 1)
            def _():
                scores(blk + 1, even_ref)
                absorb(blk, odd_ref, masked)

        scores(0, even_ref)

        @pl.loop(0, n_full)
        def _(blk):
            step(blk, False)

        @pl.loop(n_full, n_all - 1)
        def _(blk):
            step(blk, True)

        @pl.when(n_all % 2 == 1)
        def _():
            absorb(n_all - 1, even_ref, True)

        @pl.when(n_all % 2 == 0)
        def _():
            absorb(n_all - 1, odd_ref, True)

        for h in range(heads):
            at = slice(h * rows, (h + 1) * rows)
            total = jnp.sum(l_ref[at], axis=1, keepdims=True)
            obuf[r, :, h * dim:(h + 1) * dim] = (acc_ref[at] / total).astype(jnp.bfloat16)
        give.start()

    @pl.loop(0, n_req)
    def _(r):
        _, stores, give = copies(r)
        for store in stores:
            store.wait()
        give.wait()


def attention(prefix, valid, mine, far, k_cache, v_cache):
    part = (REQ, 2 * ROWS, HEAD)
    state = pltpu.VMEM((3 * 4 * ROWS, HEAD), jnp.float32)
    tile = pltpu.VMEM((3 * 4 * ROWS, BLOCK_KV), jnp.float32)
    slots = pltpu.VMEM((REQ,) + k_cache.shape[1:], jnp.bfloat16)
    q_part = pltpu.VMEM((REQ, 3, 2 * ROWS, HEAD), jnp.bfloat16)
    kv_part = pltpu.VMEM(part, jnp.bfloat16)
    return pl.pallas_call(
        attn_kernel,
        in_specs=[SMEM, SMEM] + [ANY] * 8,
        out_specs=[ANY, ANY, ANY],
        scratch_shapes=[
            slots, slots, pltpu.VMEM((REQ, 4 * ROWS, 3 * HEAD), jnp.bfloat16),
            q_part, kv_part, kv_part, q_part, kv_part, kv_part,
            pltpu.VMEM((3, 4 * ROWS, HEAD), jnp.bfloat16),
            pltpu.VMEM((WINDOW, HEAD), jnp.float32),
            state, state, state, tile, tile,
            DMA((REQ,)), DMA((REQ,)), DMA((3, REQ)), DMA((6,)),
        ],
        out_shape=[
            jax.ShapeDtypeStruct((REQ, 4 * ROWS, 3 * HEAD), jnp.bfloat16),
            jax.ShapeDtypeStruct(k_cache.shape, jnp.bfloat16),
            jax.ShapeDtypeStruct(v_cache.shape, jnp.bfloat16),
        ],
        cost_estimate=pl.CostEstimate(flops=10 ** 10, bytes_accessed=40 * 10 ** 6, transcendentals=7 * 10 ** 6),
        compiler_params=pltpu.CompilerParams(vmem_limit_bytes=67_043_328),
        name="attention",
    )(prefix, valid, *mine, *far, k_cache, v_cache)


def mlp_kernel(o_ref, x_ref, pair_ref, g_ref, wo_ref, early_ref, far_ref, wg_ref, wu_ref, wd_ref, out_ref,
               osrc, obuf, xin, wo, wg, wu, wd, hbuf, ubuf, psend, precv, pown, xsend, xrecv, x1buf, outbuf,
               w_sem, wl_sem, in_sem, o_sem, so, ro, lo, swc, rwc, sh, rh, sp, rp, ss, rs):
    dp, peers = partners()
    me, core_peer, chip_peer, far_peer = peers

    def cols(who):
        return pl.ds(pl.multiple_of(who * 384, 384), 384)

    def share(k, s):
        slot, first, n = STEPS[k]
        block = peers[s] if slot == 0 else peers[s ^ 2]
        src = (o_ref if s == 0 else osrc).at[pl.ds(first, n), block]
        dst = obuf.at[slot, pl.ds(first, n), :, cols(me)]
        if s == 0:
            return pltpu.make_async_copy(src, dst, lo.at[k])
        return send(src, dst, so.at[k, s - 1], ro.at[k, s - 1], (dp, peers[s]))

    def wo_rows(who, first, count):
        return wo.at[pl.ds(pl.multiple_of(who * 384 + first, 32), count)]

    have = (
        (wo_ref, wo_rows(me, 0, 384)),
        (early_ref, wo_rows(chip_peer, 0, WO_EARLY)),
        (far_ref, wo_rows(chip_peer, WO_EARLY, 384 - WO_EARLY)),
    )
    wo_local = tuple(pltpu.make_async_copy(src, dst, wl_sem.at[i]) for i, (src, dst) in enumerate(have))
    wo_core = tuple(send(src, dst, swc.at[i], rwc.at[i], (dp, core_peer)) for i, (src, dst) in enumerate(have))
    weights = (
        pltpu.make_async_copy(wg_ref, wg.at[pl.ds(0, FFN)], w_sem.at[0]),
        pltpu.make_async_copy(wu_ref, wu.at[pl.ds(0, FFN)], w_sem.at[1]),
        pltpu.make_async_copy(wd_ref, wd.at[pl.ds(0, FFN)], w_sem.at[2]),
    )
    x_loads = (
        pltpu.make_async_copy(x_ref, xin.at[0], in_sem.at[0]),
        pltpu.make_async_copy(pair_ref, xin.at[1], in_sem.at[1]),
    )
    steps = range(len(STEPS))

    load_o = pltpu.make_async_copy(o_ref, osrc, in_sem.at[2])
    load_o.start()
    for copy in wo_local + x_loads:
        copy.start()
    greet([(dp, core_peer), (dp, chip_peer), (dp, far_peer)])
    load_o.wait()
    for k in steps:
        for s in (2, 3, 1):
            share(k, s).start()
    for copy in wo_core:
        copy.start()
    for k in steps:
        share(k, 0).start()
    pad = jnp.zeros((FFN_PAD - FFN, WIDTH), jnp.bfloat16)
    for buf in (wg, wu, wd):
        buf[FFN:, :] = pad

    gain = g_ref[...].astype(jnp.float32).reshape(1, WIDTH)

    def half_rows(k):
        return STEPS[k][2] * ROWS

    def give_h(k):
        mine = hbuf.at[pl.ds(2 * STEP_ROWS[k], half_rows(k))]
        theirs = hbuf.at[pl.ds(2 * STEP_ROWS[k] + half_rows(k), half_rows(k))]
        return send(mine, theirs, sh.at[k], rh.at[k], (dp, core_peer))

    def part(n):
        return pl.ds(pl.multiple_of(n * HALF_WIDTH, HALF_WIDTH), HALF_WIDTH)

    def give_p(k, n):
        at = pl.ds(STEP_ROWS[k], half_rows(k))
        return send(psend.at[at, part(n)], precv.at[at, part(n)], sp.at[k, n], rp.at[k, n], (dp, core_peer))

    def give_s(k, n):
        at = pl.ds(STEPS[k][1] * ROWS, half_rows(k))
        return send(xsend.at[at, part(n)], xrecv.at[at, part(n)], ss.at[k, n], rs.at[k, n], (dp, chip_peer))

    def give_out(k, n):
        reqs = pl.ds(STEPS[k][1], STEPS[k][2])
        return pltpu.make_async_copy(outbuf.at[reqs, :, part(n)], out_ref.at[reqs, :, part(n)], o_sem.at[k, n])

    def attn_out(k):
        slot, first, n = STEPS[k]
        m = half_rows(k)
        for s in (2, 3, 1):
            share(k, s).wait_recv()
        share(k, 0).wait()
        heads = obuf[slot, first:first + n].reshape(m, WIDTH)
        attn = jnp.dot(heads, wo[...], preferred_element_type=jnp.float32).astype(jnp.bfloat16)
        base = xin[slot, first:first + n].reshape(m, WIDTH)
        mid = (base.astype(jnp.float32) + attn.astype(jnp.float32)).astype(jnp.bfloat16)
        if slot == 0:
            x1buf[first * ROWS:first * ROWS + m] = mid
        hbuf[2 * STEP_ROWS[k]:2 * STEP_ROWS[k] + m] = rms_norm(mid.astype(jnp.float32), gain)
        give_h(k).start()

    def widen(k):
        give_h(k).wait_recv()
        if k == 0:
            weights[0].wait()
            weights[1].wait()
        rows = pl.ds(2 * STEP_ROWS[k], 2 * half_rows(k))

        @pl.loop(0, FFN_PAD // FFN_TILE)
        def _(f):
            at = pl.ds(pl.multiple_of(f * FFN_TILE, FFN_TILE), FFN_TILE)
            nt = (((1,), (1,)), ((), ()))
            gate = lax.dot_general(hbuf[rows, :], wg[at, :], nt, preferred_element_type=jnp.float32)
            up = lax.dot_general(hbuf[rows, :], wu[at, :], nt, preferred_element_type=jnp.float32)
            ubuf[:2 * half_rows(k), at] = (jax.nn.silu(gate) * up).astype(jnp.bfloat16)

    def narrow(k):
        m = half_rows(k)
        at = slice(STEP_ROWS[k], STEP_ROWS[k] + m)
        if k == 0:
            weights[2].wait()

        @pl.loop(0, 2)
        def _(n):
            down = jnp.dot(ubuf[:2 * m, :], wd[:, part(n)], preferred_element_type=jnp.float32)
            pown[at, part(n)] = down[:m]
            psend[at, part(n)] = down[m:].astype(jnp.bfloat16)
            give_p(k, n).start()

    def combine(k):
        slot, first, count = STEPS[k]
        m = half_rows(k)
        at = slice(STEP_ROWS[k], STEP_ROWS[k] + m)
        mine = slice(first * ROWS, first * ROWS + m)

        @pl.loop(0, 2)
        def _(n):
            give_p(k, n).wait_recv()
            total = pown[at, part(n)] + precv[at, part(n)].astype(jnp.float32)
            if slot == 1:
                xsend[mine, part(n)] = total.astype(jnp.bfloat16)
                give_s(k, n).start()
            else:
                for j in RS_NEED[k]:
                    give_s(j, n).wait_recv()
                down = (total + xrecv[mine, part(n)].astype(jnp.float32)).astype(jnp.bfloat16)
                out = (x1buf[mine, part(n)].astype(jnp.float32) + down.astype(jnp.float32)).astype(jnp.bfloat16)
                outbuf[first:first + count, :, part(n)] = out.reshape(count, ROWS, HALF_WIDTH)
                give_out(k, n).start()

    for copy in wo_local + x_loads:
        copy.wait()
    for copy in weights:
        copy.start()
    for copy in wo_core:
        copy.wait_recv()
    attn_out(0)
    for k in steps:
        widen(k)
        if k + 1 < len(STEPS):
            attn_out(k + 1)
        if k > 0:
            combine(k - 1)
        narrow(k)
    combine(len(STEPS) - 1)
    for copy in wo_core:
        copy.wait_send()
    for k in steps:
        for s in (2, 3, 1):
            share(k, s).wait_send()
        give_h(k).wait_send()
        for n in range(2):
            give_p(k, n).wait_send()
            if STEPS[k][0] == 1:
                give_s(k, n).wait_send()
            else:
                give_out(k, n).wait()


def finish_layer(*operands):
    return pl.pallas_call(
        mlp_kernel,
        in_specs=[ANY] * 3 + [VMEM] + [ANY] * 6,
        out_specs=ANY,
        out_shape=jax.ShapeDtypeStruct((REQ, ROWS, WIDTH), jnp.bfloat16),
        scratch_shapes=[
            pltpu.VMEM((REQ, 4, ROWS, 3 * HEAD), jnp.bfloat16),
            pltpu.VMEM((2, REQ, ROWS, WIDTH), jnp.bfloat16),
            pltpu.VMEM((2, REQ, ROWS, WIDTH), jnp.bfloat16),
            pltpu.VMEM((WIDTH, WIDTH), jnp.bfloat16),
            pltpu.VMEM((FFN_PAD, WIDTH), jnp.bfloat16),
            pltpu.VMEM((FFN_PAD, WIDTH), jnp.bfloat16),
            pltpu.VMEM((FFN_PAD, WIDTH), jnp.bfloat16),
            pltpu.VMEM((2 * ALL_ROWS, WIDTH), jnp.bfloat16),
            pltpu.VMEM((MAX_ROWS, FFN_PAD), jnp.bfloat16),
            pltpu.VMEM((ALL_ROWS, WIDTH), jnp.bfloat16),
            pltpu.VMEM((ALL_ROWS, WIDTH), jnp.bfloat16),
            pltpu.VMEM((ALL_ROWS, WIDTH), jnp.float32),
            pltpu.VMEM((REQ * ROWS, WIDTH), jnp.bfloat16),
            pltpu.VMEM((REQ * ROWS, WIDTH), jnp.bfloat16),
            pltpu.VMEM((REQ * ROWS, WIDTH), jnp.bfloat16),
            pltpu.VMEM((REQ, ROWS, WIDTH), jnp.bfloat16),
            DMA((3,)), DMA((3,)), DMA((3,)), DMA((5, 2)),
            DMA((5, 3)), DMA((5, 3)), DMA((5,)),
            DMA((3,)), DMA((3,)),
            DMA((5,)), DMA((5,)), DMA((5, 2)), DMA((5, 2)), DMA((3, 2)), DMA((3, 2)),
        ],
        compiler_params=pltpu.CompilerParams(collective_id=1, has_side_effects=True, vmem_limit_bytes=62 * 1024 * 1024),
        name="finish_layer",
    )(*operands)


def solution(mesh):
    row_spec = P("dp", "tp", None)
    cache_spec = P("dp", None, "tp", None)
    req_spec = P("dp")
    rep_spec = P(None)
    col_spec = P(None, "tp")
    bias_spec = P("tp")
    down_spec = P("tp", None)

    def layer(x_rows, k_cache, v_cache, prefix, valid, g_attn, w_q, b_q, w_k, b_k, w_v, b_v, w_o, g_mlp, w_gate, w_up, w_down):
        cache_shape = (REQ, k_cache.shape[1], HEAD)
        k_old, v_old = k_cache.reshape(cache_shape), v_cache.reshape(cache_shape)
        across_chips = [(0, 2), (1, 3), (2, 0), (3, 1)]
        shared = (g_attn, b_q, b_k, b_v) + rope_tables() + (w_q, w_k, w_v)
        *qkv, x_pair, w_early, w_late = project_rows(prefix, x_rows, shared, w_o)
        mine, far = qkv[:3], qkv[3:]
        w_own, far[0] = lax.optimization_barrier((w_late, far[0]))
        w_far = lax.ppermute(w_own, "tp", across_chips)
        o, k_out, v_out = attention(prefix, valid, mine, far, k_old, v_old)
        x_out = finish_layer(o.reshape(REQ, 4, ROWS, 3 * HEAD), x_rows, x_pair, g_mlp, w_o, w_early, w_far, w_gate.T, w_up.T, w_down)
        return x_out, k_out.reshape(k_cache.shape), v_out.reshape(v_cache.shape)

    in_specs = (row_spec, cache_spec, cache_spec, req_spec, req_spec, rep_spec, col_spec, bias_spec, col_spec, bias_spec, col_spec, bias_spec, down_spec, rep_spec, col_spec, col_spec, down_spec)
    return jax.shard_map(layer, mesh=mesh, in_specs=in_specs, out_specs=(row_spec, cache_spec, cache_spec), check_vma=False)
```
